32 devices in a mesh: gz: 4 (over y, core), gy: 2 (over x), gx: 4 (over z).
Axes of the slice: x: 2, y: 2, z: 4, core: 2. Of those that a mesh axis runs over, the one named last changes fastest.
Arguments:
- positions: float32 [3, 4, 4, 32, 128], P(None, 'gx', 'gy', 'gz'), may hold values from 0 to 1
- counts: int32 [4, 4, 32], P('gx', 'gy', 'gz'), may hold values from 104 to 128
Outputs:
- energy: float32 [4, 4, 32, 128], P('gx', 'gy', 'gz')
- forces: float32 [3, 4, 4, 32, 128], P(None, 'gx', 'gy', 'gz')
The draws below stay inside these ranges and needn't reach their ends.
Inputs may be any that keep to these rules, and one draw needn't show every extreme that they name: `counts`: slot k of a cell holds an atom exactly when k < its count; positions of other slots are not used.
All inputs are finite; a program needn't handle non-finite values.
Results may differ from the reference program's by a relative error of at most 0.0003.
Values sent between devices are 32-bit elements; how exact they have to be, the bound alone decides.
A program may use at most 64 MiB of HBM per device.

```python
import jax
import jax.numpy as jnp
from jax import lax

S = 128
NX = 4
NY = 4
NZ = 32


def touch_ends(result, own_key, smallest, top_value):
    dims = result.shape
    index_at = [jax.random.randint(jax.random.fold_in(own_key, axis), (), 0, dims[axis]) for axis in range(len(dims))]
    result = result.at[tuple(index_at)].set(smallest)
    longest = dims.index(max(dims))
    index_at[longest] = (index_at[longest] + 1) % dims[longest]
    return result.at[tuple(index_at)].set(top_value)


def block_scale(key, extent, shards, least, high):
    level = 1.0
    for dim, blocks in shards:
        steps = jax.random.uniform(jax.random.fold_in(jax.random.fold_in(key, 6), dim), (blocks,), jnp.float32, least / len(shards), high / len(shards))
        level = level * jnp.repeat(jnp.exp(steps), extent[dim] // blocks).reshape((-1,) + (1,) * (len(extent) - 1 - dim))
    return level


def setup_inputs(seed: int = 0) -> dict:
    arg_keys = jax.random.split(jax.random.key(seed), 3)
    return {
        "positions": jnp.clip(1.0 * jax.random.uniform(arg_keys[0], (3, NX, NY, NZ, S), jnp.float32) ** block_scale(arg_keys[0], (3, NX, NY, NZ, S), ((1, 4), (2, 2), (3, 4)), -0.2, 0.2), 0.0, 1.0),
        "counts": touch_ends(jax.random.randint(arg_keys[1], (NX, NY, NZ), S * 13 // 16, S + 1), jax.random.fold_in(arg_keys[1], 1), S * 13 // 16, S).astype(jnp.int32),
    }


SENTINEL = 4.0
PAIR_SCALE = 0.02
EMBED_SCALE = 0.2
CUTOFF_SQUARED = 0.25
FORCE_SCALE = 8.0
neighbour_offsets = [(step_x, step_y, step_z) for step_x in (-1, 0, 1) for step_y in (-1, 0, 1) for step_z in (-1, 0, 1)]

def pair_geometry(own_cells, far_cells, offset):
    deltas = []
    for component in range(3):
        deltas.append(far_cells[component][..., None, :] - own_cells[component][..., :, None] + offset[component])
    return deltas

def density_terms(own_cells, far_cells, offset, itself):
    deltas = pair_geometry(own_cells, far_cells, offset)
    squared = deltas[0] * deltas[0] + deltas[1] * deltas[1] + deltas[2] * deltas[2]
    weight = jnp.maximum(1.0 - squared / CUTOFF_SQUARED, 0.0)
    square = weight * weight
    if itself:
        slot_count = own_cells.shape[-1]
        square = jnp.where(jnp.eye(slot_count, dtype=bool), 0.0, square)
    return (lax.optimization_barrier(jnp.sum(square, -1)), lax.optimization_barrier(jnp.sum(PAIR_SCALE * (square * square - 2.0 * square), -1)))

def force_terms(own_cells, far_cells, own_fp, far_fp, offset):
    deltas = pair_geometry(own_cells, far_cells, offset)
    squared = deltas[0] * deltas[0] + deltas[1] * deltas[1] + deltas[2] * deltas[2]
    weight = jnp.maximum(1.0 - squared / CUTOFF_SQUARED, 0.0)
    factor = (own_fp[..., :, None] + far_fp[..., None, :]) * (-2.0 * weight) + 4.0 * PAIR_SCALE * weight * (1.0 - weight * weight)
    return jnp.stack([FORCE_SCALE * lax.optimization_barrier(jnp.sum(factor * delta, -1)) for delta in deltas])

def neighbour(field, column, step_x, step_y, step_z):
    cells_x = field.shape[1]
    slab = lax.dynamic_index_in_dim(field, (column + step_x) % cells_x, 1, keepdims=False)
    return jnp.roll(slab, (-step_y, -step_z), axis=(1, 2))

def reference(positions, counts):
    slot_count = positions.shape[-1]
    occupied = jnp.arange(slot_count, dtype=jnp.int32) < counts[..., None]
    seated = jnp.where(occupied[None], positions, SENTINEL)
    cells_x = seated.shape[1]
    columns = jnp.arange(cells_x, dtype=jnp.int32)

    def slab_density(column):
        own_cells = lax.dynamic_index_in_dim(seated, column, 1, keepdims=False)
        rho_sum = jnp.zeros(own_cells.shape[1:], own_cells.dtype)
        pair_sum = jnp.zeros(own_cells.shape[1:], own_cells.dtype)
        for step_x, step_y, step_z in neighbour_offsets:
            far_cells = neighbour(seated, column, step_x, step_y, step_z)
            itself = step_x == 0 and step_y == 0 and (step_z == 0)
            rho_part, pair_part = density_terms(own_cells, far_cells, (step_x, step_y, step_z), itself)
            rho_sum = rho_sum + rho_part
            pair_sum = pair_sum + pair_part
        return jnp.stack([rho_sum, pair_sum])
    density = lax.map(slab_density, columns)
    rho_sum = density[:, 0]
    pair_sum = density[:, 1]
    fprime = -0.5 * EMBED_SCALE * lax.rsqrt(rho_sum + 1.0)
    energy = jnp.where(occupied, -EMBED_SCALE * jnp.sqrt(rho_sum + 1.0) + 0.5 * pair_sum, 0.0)
    fp_field = fprime[None]

    def slab_force(column):
        own_cells = lax.dynamic_index_in_dim(seated, column, 1, keepdims=False)
        own_fp = lax.dynamic_index_in_dim(fp_field, column, 1, keepdims=False)[0]
        pushes = jnp.zeros(own_cells.shape, own_cells.dtype)
        for step_x, step_y, step_z in neighbour_offsets:
            far_cells = neighbour(seated, column, step_x, step_y, step_z)
            far_fp = neighbour(fp_field, column, step_x, step_y, step_z)[0]
            pushes = pushes + force_terms(own_cells, far_cells, own_fp, far_fp, (step_x, step_y, step_z))
        return pushes
    forces = jnp.moveaxis(lax.map(slab_force, columns), 0, 1)
    forces = jnp.where(occupied[None], forces, 0.0)
    return (energy, forces)
```

```python
import functools

import jax
import jax.numpy as jnp
from jax import lax
from jax.experimental import pallas as pl
from jax.experimental.pallas import tpu as pltpu
from jax.sharding import PartitionSpec as P

SENTINEL = 4.0
PAIR_SCALE = 0.02
EMBED_SCALE = 0.2
FORCE_SCALE = 8.0
FAR = -1.0e6
ROWS = 8
OCTANTS = 8
HALF = 64


def split(value):
    first = value.astype(jnp.bfloat16).astype(jnp.float32)
    rest = value - first
    second = rest.astype(jnp.bfloat16).astype(jnp.float32)
    return first, second, rest - second


NAMES = ("gx", "gy", "gz")
DIRECTIONS = [
    (x, y, z) for x in (-1, 0, 1) for y in (-1, 0, 1) for z in (-1, 0, 1) if (x, y, z) != (0, 0, 0)
]
DIRECTIONS.sort(key=lambda step: -sum(abs(o) for o in step))


def device_at(counts, step):
    return {
        name: lax.rem(lax.axis_index(name) + (offset + count), count)
        for name, offset, count in zip(NAMES, step, counts)
    }


def partners(counts):
    return sorted({tuple(o % c for o, c in zip(step, counts)) for step in DIRECTIONS})


def greet(counts):
    barrier = pltpu.get_barrier_semaphore()
    for step in partners(counts):
        pl.semaphore_signal(
            barrier,
            inc=1,
            device_id=device_at(counts, step),
            device_id_type=pl.DeviceIdType.MESH,
        )


def meet(counts):
    pl.semaphore_wait(pltpu.get_barrier_semaphore(), len(partners(counts)))


def send_rims(counts, source, target, sent, landed):
    sizes = source.shape[:3]
    copies = []
    for at, step in enumerate(DIRECTIONS):
        here = tuple(
            pl.ds(0, size) if o == 0 else pl.ds(size - 1 if o > 0 else 0, 1)
            for o, size in zip(step, sizes)
        )
        there = tuple(
            pl.ds(1, size) if o == 0 else pl.ds(0 if o > 0 else size + 1, 1)
            for o, size in zip(step, sizes)
        )
        copy = pltpu.make_async_remote_copy(
            src_ref=source.at[here],
            dst_ref=target.at[there],
            send_sem=sent.at[at],
            recv_sem=landed.at[at],
            device_id=device_at(counts, step),
            device_id_type=pl.DeviceIdType.MESH,
        )
        copy.start()
        copies.append(copy)
    return copies


def arrive(copies, chosen):
    for step, copy in zip(DIRECTIONS, copies):
        if chosen(step):
            copy.wait()


def own_plane(step):
    return step[0] == 0


def side_plane(step):
    return step[0] != 0


def kernel(
    mesh_counts,
    counts_ref,
    positions,
    energy_ref,
    force_ref,
    raw,
    source,
    ext,
    far,
    far_gain,
    gain_own,
    gain_ext,
    order,
    pieces_of,
    picks,
    weights,
    wide_rows,
    dense,
    gains,
    table_rows,
    table,
    raw_sem,
    table_sem,
    sent,
    landed,
    gain_sent,
    gain_landed,
):
    sizes = source.shape[:3]
    sx, sy, sz = sizes
    wide = ext.shape[:3]
    wx, wy, wz = wide
    slots = source.shape[-1]
    cells = sx * sy * sz
    group_count = weights.shape[1]
    depth = picks.shape[1]
    plane = wy * wz

    greet(mesh_counts)
    fetch = pltpu.make_async_copy(positions, raw, raw_sem)
    fetch.start()

    lane = lax.broadcasted_iota(jnp.int32, (cells, slots), 1)
    cell = lax.broadcasted_iota(jnp.int32, (cells, slots), 0)
    occupancy = jnp.zeros((cells, slots), jnp.int32)
    for x in range(sx):
        for y in range(sy):
            for z in range(sz):
                occupancy = jnp.where(cell == (x * sy + y) * sz + z, counts_ref[x, y, z], occupancy)
    filled = lane < occupancy
    column_of = sum(((cell >= k * sz).astype(jnp.int32) for k in range(1, sx * sy)), jnp.zeros_like(cell))
    plane_of = sum(((column_of >= k * sy).astype(jnp.int32) for k in range(1, sx)), jnp.zeros_like(cell))
    spots = (plane_of, column_of - plane_of * sy, cell - column_of * sz)

    fetch.wait()
    seated = [
        jnp.where(filled, raw[k].reshape(cells, slots), SENTINEL) for k in range(3)
    ]
    for k in range(3):
        source[:, :, :, k, :] = seated[k].reshape(sizes + (slots,))
    source[:, :, :, 3, :] = jnp.zeros(sizes + (slots,), jnp.float32)

    meet(mesh_counts)
    copies = send_rims(mesh_counts, source, ext, sent, landed)

    own = [
        jnp.where(
            filled,
            seated[k] + ((spots[k] + 1).astype(jnp.float32) - 0.5 * wide[k]),
            0.0,
        )
        for k in range(3)
    ]
    inner = tuple(slice(1, 1 + size) for size in sizes)
    ext[inner] = source[...]

    upper = [(seated[k] >= 0.5).astype(jnp.int32) for k in range(3)]
    octant = jnp.where(filled, 4 * upper[0] + 2 * upper[1] + upper[2], OCTANTS)
    members = jnp.concatenate(
        [jnp.where(octant == o, 1.0, 0.0) for o in range(OCTANTS)], axis=0
    ).astype(jnp.bfloat16)
    before = lax.broadcasted_iota(jnp.int32, (slots, 2 * slots), 0)
    after = lax.broadcasted_iota(jnp.int32, (slots, 2 * slots), 1)
    earlier = jnp.where((after >= slots) | (before < after), 1.0, 0.0).astype(jnp.bfloat16)
    ranks = jnp.dot(members, earlier, preferred_element_type=jnp.float32).astype(jnp.int32)
    start = jnp.zeros((cells, slots), jnp.int32)
    place = jnp.full((cells, slots), -1, jnp.int32)
    block = jnp.zeros((cells, slots), jnp.int32)
    group = jnp.where(lane >= HALF, lane - HALF, lane)
    for o in range(OCTANTS):
        rows = ranks[o * cells : (o + 1) * cells]
        place = jnp.where(octant == o, start + rows[:, :slots], place)
        if o:
            block = block + jnp.where(group * ROWS >= start, 1, 0)
        start = start + ((rows[:, slots:] + (ROWS - 1)) & -ROWS)
    order[...] = place
    corner = (
        ((spots[0] + 1) * wy + spots[1] + ((block >> 1) & 1)) * wz + spots[2] + (block & 1)
    )
    table_rows[...] = jnp.where(lane >= HALF, corner + (2 * (block >> 2) - 1) * plane, corner)
    tabulate = pltpu.make_async_copy(table_rows, table, table_sem)
    tabulate.start()

    near = 1.0 - 4.0 * (own[0] * own[0] + own[1] * own[1] + own[2] * own[2])
    for k, value in enumerate([8.0 * own[0], 8.0 * own[1], 8.0 * own[2], near]):
        for part, piece in enumerate(split(value)):
            pieces_of[part, k] = piece

    slot_lane = lax.broadcasted_iota(jnp.int32, (ROWS, slots), 1)

    def spread(column):
        return jnp.broadcast_to(column, (ROWS, slots))

    batch = next(n for n in (4, 2, 1) if cells % n == 0)

    def sort_cells(i, carry):
        found = []
        for j in range(batch):
            c = i * batch + j
            spot = order[pl.ds(c, 1), :]
            target = lax.broadcasted_iota(jnp.int32, (depth, slots), 0)
            pick = jnp.where(target == spot, 1.0, 0.0).astype(jnp.bfloat16)
            picks[c] = pick
            pieces = []
            for part in range(3):
                rows = [pieces_of[part, k, pl.ds(c, 1), :] for k in range(4)]
                pieces.append(jnp.concatenate(rows + [jnp.zeros((4, slots), jnp.float32)], axis=0))
            values = jnp.concatenate(pieces, axis=1).astype(jnp.bfloat16)
            found.append(
                lax.dot_general(
                    jnp.concatenate([pick, pick, pick], axis=1),
                    values,
                    (((1,), (1,)), ((), ())),
                    preferred_element_type=jnp.float32,
                )
            )
        for k in range(4):
            for j in range(batch):
                for g in range(group_count):
                    wide_rows[i * batch + j, g, k] = spread(
                        found[j][g * ROWS : (g + 1) * ROWS, k : k + 1]
                    )
        return carry

    lax.fori_loop(0, cells // batch, sort_cells, 0)

    def prepare(x, y):
        tile = ext[x, y]
        shape = (wz, ROWS, slots)
        rows = [jnp.broadcast_to(tile[:, k : k + 1, :], shape) for k in range(3)]
        there = rows[0] < 2.0
        floor = lax.broadcasted_iota(jnp.int32, shape, 0).astype(jnp.float32) - 0.5 * wz
        shifts = (
            lax.convert_element_type(x, jnp.float32) - 0.5 * wx,
            lax.convert_element_type(y, jnp.float32) - 0.5 * wy,
            floor,
        )
        coords = [jnp.where(there, row + shift, 0.0) for row, shift in zip(rows, shifts)]
        squares = coords[0] * coords[0] + coords[1] * coords[1] + coords[2] * coords[2]
        at = pl.ds((x * wy + y) * wz, wz)
        for k in range(3):
            far[at, k] = coords[k]
        far[at, 3] = jnp.where(there, -4.0 * squares, FAR)

    def prepare_gain(x, y):
        far_gain[pl.ds((x * wy + y) * wz, wz)] = jnp.broadcast_to(
            gain_ext[x, y], (wz, ROWS, slots)
        )

    def own_columns(body):
        def step(i, carry):
            body(i // wy + 1, i % wy)
            return carry

        lax.fori_loop(0, sx * wy, step, 0)

    def side_columns(body):
        def step(i, carry):
            body(i // wy * (wx - 1), i % wy)
            return carry

        lax.fori_loop(0, 2 * wy, step, 0)

    dense[...] = jnp.zeros_like(dense)

    def density(phase):
        def one_cell(c, carry):
            def one_group(g, inside):
                base = table[c, phase * HALF + g]
                xi, yi, zi, ci = (wide_rows[c, g, k] for k in range(4))
                if phase:
                    rho, quartic = wide_rows[c, g, 4], wide_rows[c, g, 5]
                else:
                    rho, quartic = (jnp.zeros((ROWS, slots), jnp.float32),) * 2
                for dy in range(2):
                    for dz in range(2):
                        at = base + (dy * wz + dz)
                        t = (far[at, 3] + ci) + xi * far[at, 0]
                        t = t + yi * far[at, 1] + zi * far[at, 2]
                        w = jnp.maximum(t, 0.0)
                        weights[c, g, 4 * phase + 2 * dy + dz] = w
                        s = w * w
                        rho = rho + s
                        quartic = quartic + s * s
                if phase:
                    first = jnp.sum(rho, axis=1, keepdims=True)
                    second = jnp.sum(quartic, axis=1, keepdims=True)
                    at = pl.ds(g * ROWS, ROWS)
                    dense[at, :] = jnp.where(
                        slot_lane == c,
                        first,
                        jnp.where(slot_lane == cells + c, second, dense[at, :]),
                    )
                else:
                    wide_rows[c, g, 4] = rho
                    wide_rows[c, g, 5] = quartic
                return inside

            lax.fori_loop(0, group_count, one_group, 0, unroll=True)
            return carry

        lax.fori_loop(0, cells, one_cell, 0)

    def unsort(value, kinds):
        turned = value.T[: kinds * cells, :depth]
        pieces = jnp.concatenate(split(turned), axis=0).astype(jnp.bfloat16)
        total = jnp.zeros((3 * kinds * cells, slots), jnp.float32)
        row = lax.broadcasted_iota(jnp.int32, pieces.shape, 0) % cells
        for c in range(cells):
            kept = jnp.where(row == c, pieces, jnp.zeros_like(pieces))
            total = total + jnp.dot(kept, picks[c], preferred_element_type=jnp.float32)
        size = kinds * cells
        return total[:size] + total[size : 2 * size] + total[2 * size :]

    arrive(copies, own_plane)
    own_columns(prepare)
    tabulate.wait()
    density(0)
    arrive(copies, side_plane)
    side_columns(prepare)
    density(1)

    first = jnp.maximum(dense[...] - 1.0, 0.0)
    second = pltpu.roll(first, slots - cells, 1)
    pair_sum = PAIR_SCALE * (second - 2.0 * first)
    energy = -EMBED_SCALE * jnp.sqrt(first + 1.0) + 0.5 * pair_sum
    fprime = -0.5 * EMBED_SCALE * lax.rsqrt(first + 1.0)
    gain = 0.5 - fprime * (0.5 / PAIR_SCALE)
    gains[...] = gain
    gain_rows = unsort(gain, 1)
    gain_own[...] = gain_rows.reshape(sizes + (1, slots))
    copies = send_rims(mesh_counts, gain_own, gain_ext, gain_sent, gain_landed)
    gain_ext[inner] = gain_rows.reshape(sizes + (1, slots))
    energy_rows = unsort(energy, 1)
    energy_ref[...] = jnp.where(filled, energy_rows, 0.0).reshape(sizes + (slots,))
    dense[...] = jnp.zeros_like(dense)

    def force(phase):
        def one_cell(c, carry):
            def one_group(g, inside):
                base = table[c, phase * HALF + g]
                rows = pl.ds(g * ROWS, ROWS)
                gi = wide_rows[c, g, 4]
                if phase:
                    parts = [wide_rows[c, g, k] for k in range(4)]
                else:
                    parts = [jnp.zeros((ROWS, slots), jnp.float32)] * 4
                for dy in range(2):
                    for dz in range(2):
                        at = base + (dy * wz + dz)
                        w = weights[c, g, 4 * phase + 2 * dy + dz]
                        f = w * ((far_gain[at] + gi) - w * w)
                        parts[0] = parts[0] + f
                        for k in range(3):
                            parts[k + 1] = parts[k + 1] + f * far[at, k]
                if phase:
                    kept = dense[rows, :]
                    for k in range(4):
                        kept = jnp.where(
                            slot_lane == k * cells + c,
                            jnp.sum(parts[k], axis=1, keepdims=True),
                            kept,
                        )
                    dense[rows, :] = kept
                else:
                    for k in range(4):
                        wide_rows[c, g, k] = parts[k]
                return inside

            lax.fori_loop(0, group_count, one_group, 0, unroll=True)
            return carry

        lax.fori_loop(0, cells, one_cell, 0)

    def spread_gains(g, carry):
        tile = gains[pl.ds(g * ROWS, ROWS), :]
        for c in range(cells):
            wide_rows[c, g, 4] = spread(tile[:, c : c + 1])
        return carry

    lax.fori_loop(0, group_count, spread_gains, 0)
    arrive(copies, own_plane)
    own_columns(prepare_gain)
    force(0)
    arrive(copies, side_plane)
    side_columns(prepare_gain)
    force(1)

    moments = unsort(dense[...], 4)
    scale = FORCE_SCALE * 4.0 * PAIR_SCALE
    for k in range(3):
        push = moments[(k + 1) * cells : (k + 2) * cells] - own[k] * moments[:cells]
        force_ref[k] = jnp.where(filled, scale * push, 0.0).reshape(sizes + (slots,))


def per_device(mesh_counts, positions, counts):
    slots = positions.shape[-1]
    sizes = positions.shape[1:4]
    wide = tuple(size + 2 for size in sizes)
    cells = sizes[0] * sizes[1] * sizes[2]
    far_cells = wide[0] * wide[1] * wide[2]
    groups = (slots + OCTANTS * (ROWS - 1)) // ROWS
    depth = -(-groups // 2) * 2 * ROWS
    tall = -(-depth // 128) * 128
    f32 = jnp.float32
    return pl.pallas_call(
        functools.partial(kernel, mesh_counts),
        out_shape=(
            jax.ShapeDtypeStruct(sizes + (slots,), f32),
            jax.ShapeDtypeStruct((3,) + sizes + (slots,), f32),
        ),
        in_specs=[
            pl.BlockSpec(memory_space=pltpu.SMEM),
            pl.BlockSpec(memory_space=pl.ANY),
        ],
        out_specs=(pl.BlockSpec(memory_space=pltpu.VMEM),) * 2,
        scratch_shapes=[
            pltpu.VMEM((3,) + sizes + (slots,), f32),
            pltpu.VMEM(sizes + (4, slots), f32),
            pltpu.VMEM(wide + (4, slots), f32),
            pltpu.VMEM((far_cells, 4, ROWS, slots), f32),
            pltpu.VMEM((far_cells, ROWS, slots), f32),
            pltpu.VMEM(sizes + (1, slots), f32),
            pltpu.VMEM(wide + (1, slots), f32),
            pltpu.VMEM((cells, slots), jnp.int32),
            pltpu.VMEM((3, 4, cells, slots), f32),
            pltpu.VMEM((cells, depth, slots), jnp.bfloat16),
            pltpu.VMEM((cells, groups, 8, ROWS, slots), f32),
            pltpu.VMEM((cells, groups, 6, ROWS, slots), f32),
            pltpu.VMEM((tall, slots), f32),
            pltpu.VMEM((tall, slots), f32),
            pltpu.VMEM((cells, slots), jnp.int32),
            pltpu.SMEM((cells, slots), jnp.int32),
            pltpu.SemaphoreType.DMA,
            pltpu.SemaphoreType.DMA,
        ]
        + [pltpu.SemaphoreType.DMA((len(DIRECTIONS),))] * 4,
        compiler_params=pltpu.CompilerParams(collective_id=0, has_side_effects=True),
        name="atoms",
    )(counts, positions)


def solution(mesh):
    placed = (P(None, "gx", "gy", "gz", None), P("gx", "gy", "gz"))
    return jax.shard_map(
        functools.partial(per_device, tuple(mesh.shape[name] for name in NAMES)),
        mesh=mesh,
        in_specs=placed,
        out_specs=(P("gx", "gy", "gz", None), P(None, "gx", "gy", "gz", None)),
        check_vma=False,
    )
```

```python
import functools
import math

import jax
import jax.numpy as jnp
from jax import lax
from jax.experimental import pallas as pl
from jax.experimental.pallas import tpu as pltpu
from jax.sharding import PartitionSpec as P

SENTINEL = 4.0
PAIR_SCALE = 0.02
EMBED_SCALE = 0.2
FORCE_SCALE = 8.0
FAR = -1.0e6
ROWS = 8
OCTANTS = 8
SPAN = 32


def split(value):
    first = value.astype(jnp.bfloat16).astype(jnp.float32)
    rest = value - first
    second = rest.astype(jnp.bfloat16).astype(jnp.float32)
    return first, second, rest - second


NAMES = ("gx", "gy", "gz")
DIRECTIONS = [
    (x, y, z) for x in (-1, 0, 1) for y in (-1, 0, 1) for z in (-1, 0, 1) if (x, y, z) != (0, 0, 0)
]
DIRECTIONS.sort(key=lambda step: (abs(step[0]) * (1 + abs(step[1])), -sum(map(abs, step))))


def device_at(counts, step):
    return {
        name: lax.rem(lax.axis_index(name) + (offset + count), count)
        for name, offset, count in zip(NAMES, step, counts)
    }


def partners(counts):
    return sorted({tuple(o % c for o, c in zip(step, counts)) for step in DIRECTIONS})


def greet(counts):
    barrier = pltpu.get_barrier_semaphore()
    for step in partners(counts):
        pl.semaphore_signal(
            barrier,
            inc=1,
            device_id=device_at(counts, step),
            device_id_type=pl.DeviceIdType.MESH,
        )


def meet(counts):
    pl.semaphore_wait(pltpu.get_barrier_semaphore(), len(partners(counts)))


def send_rims(counts, source, target, sent, landed):
    lead = (slice(None),) * (source.ndim - 5)
    sizes = source.shape[-5:-2]
    copies = []
    for at, step in enumerate(DIRECTIONS):
        here = tuple(
            pl.ds(0, size) if o == 0 else pl.ds(size - 1 if o > 0 else 0, 1)
            for o, size in zip(step, sizes)
        )
        there = tuple(
            pl.ds(1, size) if o == 0 else pl.ds(0 if o > 0 else size + 1, 1)
            for o, size in zip(step, sizes)
        )
        copy = pltpu.make_async_remote_copy(
            src_ref=source.at[lead + here],
            dst_ref=target.at[lead + there],
            send_sem=sent.at[at],
            recv_sem=landed.at[at],
            device_id=device_at(counts, step),
            device_id_type=pl.DeviceIdType.MESH,
        )
        copy.start()
        copies.append(copy)
    return copies


def arrive(copies, chosen):
    for step, copy in zip(DIRECTIONS, copies):
        if chosen(step):
            copy.wait()


def own_plane(step):
    return step[0] == 0


def side_faces(step):
    return step[0] != 0 and step[1] == 0


def side_edges(step):
    return step[0] != 0 and step[1] != 0


def halves(value):
    high = value.astype(jnp.bfloat16)
    return high, (value - high.astype(jnp.float32)).astype(jnp.bfloat16)


def kernel(
    mesh_counts,
    counts,
    positions,
    energy_ref,
    force_ref,
    held,
    raw,
    source,
    ext,
    far,
    far_gain,
    gain_own,
    gain_ext,
    order,
    pieces_of,
    picks,
    weights,
    lanes_of,
    dense,
    table_rows,
    table,
    fetch_sem,
    table_sem,
    sent,
    landed,
    gain_sent,
    gain_landed,
):
    sizes = gain_own.shape[:3]
    sx, sy, sz = sizes
    wide = gain_ext.shape[:3]
    wx, wy, wz = wide
    slots = source.shape[-1]
    cells = sx * sy * sz
    group_count = weights.shape[1]
    depth = picks.shape[1]
    plane = wy * wz

    fetches = [
        pltpu.make_async_copy(counts, held, fetch_sem.at[0]),
        pltpu.make_async_copy(positions, raw, fetch_sem.at[1]),
    ]
    for fetch in fetches:
        fetch.start()
    greet(mesh_counts)

    lane = lax.broadcasted_iota(jnp.int32, (cells, slots), 1)
    cell = lax.broadcasted_iota(jnp.int32, (cells, slots), 0)
    column_of = sum(((cell >= k * sz).astype(jnp.int32) for k in range(1, sx * sy)), jnp.zeros_like(cell))
    plane_of = sum(((column_of >= k * sy).astype(jnp.int32) for k in range(1, sx)), jnp.zeros_like(cell))
    spots = (plane_of, column_of - plane_of * sy, cell - column_of * sz)

    for fetch in fetches:
        fetch.wait()
    occupancy = jnp.zeros((cells, slots), jnp.int32)
    for x in range(sx):
        for y in range(sy):
            for z in range(sz):
                occupancy = jnp.where(cell == (x * sy + y) * sz + z, held[x, y, z], occupancy)
    filled = lane < occupancy
    seated = [
        jnp.where(filled, raw[k].reshape(cells, slots), SENTINEL) for k in range(3)
    ]
    for k in range(3):
        source[k] = seated[k].reshape(sizes + (1, slots))

    meet(mesh_counts)
    copies = send_rims(mesh_counts, source, ext, sent, landed)

    own = [
        jnp.where(
            filled,
            seated[k] + ((spots[k] + 1).astype(jnp.float32) - 0.5 * wide[k]),
            0.0,
        )
        for k in range(3)
    ]
    inner = tuple(slice(1, 1 + size) for size in sizes)
    for k in range(3):
        ext[(k,) + inner] = seated[k].reshape(sizes + (1, slots))

    upper = [(seated[k] >= 0.5).astype(jnp.int32) for k in range(3)]
    octant = jnp.where(filled, 4 * upper[0] + 2 * upper[1] + upper[2], OCTANTS)
    members = jnp.concatenate(
        [jnp.where(octant == o, 1.0, 0.0) for o in range(OCTANTS)], axis=0
    ).astype(jnp.bfloat16)
    before = lax.broadcasted_iota(jnp.int32, (slots, 2 * slots), 0)
    after = lax.broadcasted_iota(jnp.int32, (slots, 2 * slots), 1)
    earlier = jnp.where((after >= slots) | (before < after), 1.0, 0.0).astype(jnp.bfloat16)
    ranks = jnp.dot(members, earlier, preferred_element_type=jnp.float32).astype(jnp.int32)
    start = jnp.zeros((cells, slots), jnp.int32)
    place = jnp.full((cells, slots), -1, jnp.int32)
    block = jnp.zeros((cells, slots), jnp.int32)
    phase_of = lane // SPAN
    group = lane - phase_of * SPAN
    for o in range(OCTANTS):
        rows = ranks[o * cells : (o + 1) * cells]
        place = jnp.where(octant == o, start + rows[:, :slots], place)
        if o:
            block = block + jnp.where(group * ROWS >= start, 1, 0)
        start = start + ((rows[:, slots:] + (ROWS - 1)) & -ROWS)
    order[...] = place
    bits = [(block >> 2) & 1, (block >> 1) & 1, block & 1]
    far_x = jnp.where(phase_of >= 2, spots[0] + 2 * bits[0], spots[0] + 1)
    far_y = jnp.where((phase_of & 1) == 1, spots[1] + 2 * bits[1], spots[1] + 1)
    table_rows[...] = (far_x * wy + far_y) * wz + spots[2] + bits[2]
    tabulate = pltpu.make_async_copy(table_rows, table, table_sem)
    tabulate.start()

    near = 1.0 - 4.0 * (own[0] * own[0] + own[1] * own[1] + own[2] * own[2])
    for k, value in enumerate([8.0 * own[0], 8.0 * own[1], 8.0 * own[2], near]):
        for part, piece in enumerate(split(value)):
            pieces_of[part, k] = piece

    batch = next(n for n in (8, 4, 2, 1) if cells % n == 0)
    kind_row = lax.broadcasted_iota(jnp.int32, (16, 4 * slots), 0)
    kind_lane = lax.broadcasted_iota(jnp.int32, (16, 4 * slots), 1)
    smear = jnp.where(
        (kind_row < 12) & ((kind_row & 3) == kind_lane // slots), 1.0, 0.0
    ).astype(jnp.bfloat16)

    def sort_cells(i, carry):
        found = []
        for j in range(batch):
            c = i * batch + j
            spot = order[pl.ds(c, 1), :]
            target = lax.broadcasted_iota(jnp.int32, (depth, slots), 0)
            pick = jnp.where(target == spot, 1.0, 0.0).astype(jnp.bfloat16)
            picks[c] = pick
            rows = [pieces_of[part, k, pl.ds(c, 1), :] for part in range(3) for k in range(4)]
            rows += [jnp.zeros((4, slots), jnp.float32)]
            found.append(
                lax.dot_general(
                    pick,
                    jnp.concatenate(rows, axis=0).astype(jnp.bfloat16),
                    (((1,), (1,)), ((), ())),
                    preferred_element_type=jnp.float32,
                ).astype(jnp.bfloat16)
            )
        for j in range(batch):
            spread = jnp.dot(found[j], smear, preferred_element_type=jnp.float32)
            for k in range(4):
                for g in range(group_count):
                    lanes_of[i * batch + j, g, k] = spread[
                        g * ROWS : (g + 1) * ROWS, k * slots : (k + 1) * slots
                    ]
        return carry

    lax.fori_loop(0, cells // batch, sort_cells, 0)

    def prepare(x, y, z, count):
        shape = (count, ROWS, slots)
        rows = [jnp.broadcast_to(ext[k, x, y, pl.ds(z, count)], shape) for k in range(3)]
        there = rows[0] < 2.0
        floor = lax.broadcasted_iota(jnp.int32, shape, 0).astype(jnp.float32) + (z - 0.5 * wz)
        shifts = (
            lax.convert_element_type(x, jnp.float32) - 0.5 * wx,
            lax.convert_element_type(y, jnp.float32) - 0.5 * wy,
            floor,
        )
        coords = [jnp.where(there, row + shift, 0.0) for row, shift in zip(rows, shifts)]
        squares = coords[0] * coords[0] + coords[1] * coords[1] + coords[2] * coords[2]
        at = pl.ds((x * wy + y) * wz + z, count)
        for k in range(3):
            far[at, k] = coords[k]
        far[at, 3] = jnp.where(there, -4.0 * squares, FAR)

    def prepare_gain(x, y, z, count):
        far_gain[pl.ds((x * wy + y) * wz + z, count)] = jnp.broadcast_to(
            gain_ext[x, y, pl.ds(z, count)], (count, ROWS, slots)
        )

    def columns(count, where, body):
        def step(i, carry):
            body(*where(i))
            return carry

        lax.fori_loop(0, count, step, 0)

    def inner_columns(body):
        columns(sx * sy, lambda i: (i // sy + 1, i % sy + 1), lambda x, y: body(x, y, 1, sz))

    def plane_columns(body):
        def ends(x, y):
            body(x, y, 0, 1)
            body(x, y, wz - 1, 1)

        columns(sx * sy, lambda i: (i // sy + 1, i % sy + 1), ends)
        columns(
            2 * sx, lambda i: (i // 2 + 1, i % 2 * (wy - 1)), lambda x, y: body(x, y, 0, wz)
        )

    def side_columns(ys, count, body):
        columns(
            2 * count,
            lambda i: (i // count * (wx - 1), ys(i % count)),
            lambda x, y: body(x, y, 0, wz),
        )

    def face_columns(body):
        side_columns(lambda y: y + 1, sy, body)

    def edge_columns(body):
        side_columns(lambda y: y * (wy - 1), 2, body)

    slot_lane = lax.broadcasted_iota(jnp.int32, (ROWS, slots), 1)

    def lane_sums(c, rows, parts):
        kept = dense[rows, :]
        for k, part in enumerate(parts):
            kept = jnp.where(
                slot_lane == k * cells + c, jnp.sum(part, axis=1, keepdims=True), kept
            )
        dense[rows, :] = kept

    def sorted_rows(kinds):
        flat = dense[...].T
        return [flat[k * cells : (k + 1) * cells, :depth] for k in range(kinds)]

    def all_cells(body, *phases):
        columns(cells, lambda i: (i,), lambda c: body(c, phases))

    def last_cells(body, *phases):
        several = next(n for n in (4, 2, 1) if cells % n == 0)

        def step(i, carry):
            for j in range(several):
                body(i * several + j, phases)
            return carry

        lax.fori_loop(0, cells // several, step, 0)

    def middle_cells(body):
        span = sz - 2
        if span > 0:
            columns(
                sx * sy * span,
                lambda i: (i // span * sz + 1 + i % span,),
                lambda c: body(c, (0,)),
            )

    def end_cells(body):
        ends = min(sz, 2)
        columns(
            ends * sx * sy,
            lambda i: (i // ends * sz + i % ends * (sz - 1),),
            lambda c: body(c, (0,)),
        )

    def density(c, phases):
        def one_group(g, inside):
            xi, yi, zi, ci = (lanes_of[c, g, k] for k in range(4))
            if phases[0]:
                rho, quartic = lanes_of[c, g, 4], lanes_of[c, g, 5]
            else:
                rho, quartic = (jnp.zeros((ROWS, slots), jnp.float32),) * 2
            for phase in phases:
                base = table[c, phase * SPAN + g]
                for step in range(2):
                    at = base + step
                    t = (far[at, 3] + ci) + xi * far[at, 0]
                    t = t + yi * far[at, 1] + zi * far[at, 2]
                    w = jnp.maximum(t, 0.0)
                    weights[c, g, 2 * phase + step] = w
                    s = w * w
                    rho = rho + s
                    quartic = quartic + s * s
            if phases[-1] == 3:
                lane_sums(c, pl.ds(g * ROWS, ROWS), (rho, quartic))
            else:
                lanes_of[c, g, 4] = rho
                lanes_of[c, g, 5] = quartic
            return inside

        lax.fori_loop(0, group_count, one_group, 0, unroll=True)

    def force(c, phases):
        def one_group(g, inside):
            gi = lanes_of[c, g, 3]
            if phases[0]:
                parts = [lanes_of[c, g, 4 + k] for k in range(4)]
            else:
                parts = [jnp.zeros((ROWS, slots), jnp.float32)] * 4
            for phase in phases:
                base = table[c, phase * SPAN + g]
                for step in range(2):
                    at = base + step
                    w = weights[c, g, 2 * phase + step]
                    f = w * ((far_gain[at] + gi) - w * w)
                    for k in range(3):
                        parts[k] = parts[k] + f * far[at, k]
                    parts[3] = parts[3] + f
            if phases[-1] == 3:
                whole = 0.125 * parts[3]
                parts = [parts[k] - lanes_of[c, g, k] * whole for k in range(3)]
                lane_sums(c, pl.ds(g * ROWS, ROWS), parts)
            else:
                for k in range(4):
                    lanes_of[c, g, 4 + k] = parts[k]
            return inside

        lax.fori_loop(0, group_count, one_group, 0, unroll=True)

    def unsort(kinds):
        pieces = [piece for value in kinds for piece in halves(value)]
        pieces = jnp.concatenate(pieces, axis=0)
        total = jnp.zeros((2 * len(kinds) * cells, slots), jnp.float32)
        row = lax.broadcasted_iota(jnp.int32, pieces.shape, 0) % cells
        for c in range(cells):
            kept = jnp.where(row == c, pieces, jnp.zeros_like(pieces))
            total = total + jnp.dot(kept, picks[c], preferred_element_type=jnp.float32)
        rows = [total[k * cells : (k + 1) * cells] for k in range(2 * len(kinds))]
        return [rows[2 * k] + rows[2 * k + 1] for k in range(len(kinds))]

    dense[...] = jnp.zeros_like(dense)
    inner_columns(prepare)
    tabulate.wait()
    middle_cells(density)
    arrive(copies, own_plane)
    plane_columns(prepare)
    end_cells(density)
    all_cells(density, 1)
    arrive(copies, side_faces)
    face_columns(prepare)
    all_cells(density, 2)
    arrive(copies, side_edges)
    edge_columns(prepare)
    last_cells(density, 3)

    rho_rows, quartic_rows = sorted_rows(2)
    first = jnp.maximum(rho_rows - 1.0, 0.0)
    second = jnp.maximum(quartic_rows - 1.0, 0.0)
    fprime = -0.5 * EMBED_SCALE * lax.rsqrt(first + 1.0)
    gain = 0.5 - fprime * (0.5 / PAIR_SCALE)
    gain_rows = unsort([gain])[0]
    gain_own[...] = gain_rows.reshape(sizes + (1, slots))
    copies = send_rims(mesh_counts, gain_own, gain_ext, gain_sent, gain_landed)
    gain_ext[inner] = gain_rows.reshape(sizes + (1, slots))
    pair_sum = PAIR_SCALE * (second - 2.0 * first)
    energy = -EMBED_SCALE * jnp.sqrt(first + 1.0) + 0.5 * pair_sum
    energy_rows = unsort([energy])[0]
    energy_ref[...] = jnp.where(filled, energy_rows, 0.0).reshape(sizes + (slots,))

    tall = [piece.astype(jnp.float32) for piece in halves(gain)]
    tall += [jnp.zeros((slots - 2 * cells, depth), jnp.float32)]
    tall = jnp.concatenate(tall, axis=0)
    tall = jnp.concatenate([tall, jnp.zeros((slots, -depth % 128), jnp.float32)], axis=1)
    standing = tall.T[:depth].astype(jnp.bfloat16)
    pair = 2 if cells % 2 == 0 else 1
    pick_row = lax.broadcasted_iota(jnp.int32, (slots, pair * slots), 0)
    pick_cell = jnp.where(
        pick_row < 2 * cells, pick_row - jnp.where(pick_row >= cells, cells, 0), -1
    )
    pick_lane = lax.broadcasted_iota(jnp.int32, (slots, pair * slots), 1) // slots
    for i in range(cells // pair):
        chosen = jnp.where(pick_cell == pair * i + pick_lane, 1.0, 0.0).astype(jnp.bfloat16)
        spread = jnp.dot(standing, chosen, preferred_element_type=jnp.float32)
        for j in range(pair):
            for g in range(group_count):
                lanes_of[pair * i + j, g, 3] = spread[
                    g * ROWS : (g + 1) * ROWS, j * slots : (j + 1) * slots
                ]

    inner_columns(prepare_gain)
    middle_cells(force)
    arrive(copies, own_plane)
    plane_columns(prepare_gain)
    end_cells(force)
    all_cells(force, 1)
    arrive(copies, side_faces)
    arrive(copies, side_edges)
    face_columns(prepare_gain)
    edge_columns(prepare_gain)
    last_cells(force, 2, 3)

    scale = FORCE_SCALE * 4.0 * PAIR_SCALE
    for k, push in enumerate(unsort(sorted_rows(3))):
        force_ref[k] = jnp.where(filled, scale * push, 0.0).reshape(sizes + (slots,))


def per_device(mesh_counts, positions, counts):
    slots = positions.shape[-1]
    sizes = positions.shape[1:4]
    wide = tuple(size + 2 for size in sizes)
    cells = sizes[0] * sizes[1] * sizes[2]
    far_cells = wide[0] * wide[1] * wide[2]
    groups = (slots + OCTANTS * (ROWS - 1)) // ROWS
    depth = -(-groups // 2) * 2 * ROWS
    f32, bf16, i32 = jnp.float32, jnp.bfloat16, jnp.int32
    vmem = [
        ((3,) + sizes + (slots,), f32),
        ((3,) + sizes + (1, slots), f32),
        ((3,) + wide + (1, slots), f32),
        ((far_cells, 4, ROWS, slots), f32),
        ((far_cells, ROWS, slots), f32),
        (sizes + (1, slots), f32),
        (wide + (1, slots), f32),
        ((cells, slots), i32),
        ((3, 4, cells, slots), f32),
        ((cells, depth, slots), bf16),
        ((cells, groups, 8, ROWS, slots), f32),
        ((cells, groups, 8, ROWS, slots), f32),
        ((-(-depth // 128) * 128, slots), f32),
        ((cells, slots), i32),
    ]
    held = sum(math.prod(shape) * jnp.dtype(kind).itemsize for shape, kind in vmem)
    return pl.pallas_call(
        functools.partial(kernel, mesh_counts),
        out_shape=(
            jax.ShapeDtypeStruct(sizes + (slots,), f32),
            jax.ShapeDtypeStruct((3,) + sizes + (slots,), f32),
        ),
        in_specs=[pl.BlockSpec(memory_space=pltpu.HBM)] * 2,
        out_specs=(pl.BlockSpec(memory_space=pltpu.VMEM),) * 2,
        scratch_shapes=[pltpu.SMEM(counts.shape, i32)]
        + [pltpu.VMEM(shape, kind) for shape, kind in vmem]
        + [
            pltpu.SMEM((cells, slots), i32),
            pltpu.SemaphoreType.DMA((2,)),
            pltpu.SemaphoreType.DMA,
        ]
        + [pltpu.SemaphoreType.DMA((len(DIRECTIONS),))] * 4,
        compiler_params=pltpu.CompilerParams(
            collective_id=0,
            has_side_effects=True,
            vmem_limit_bytes=held + (4 << 20),
        ),
        name="atoms",
    )(*(pltpu.with_memory_space_constraint(x, pltpu.HBM) for x in (counts, positions)))


def solution(mesh):
    placed = (P(None, "gx", "gy", "gz", None), P("gx", "gy", "gz"))
    return jax.shard_map(
        functools.partial(per_device, tuple(mesh.shape[name] for name in NAMES)),
        mesh=mesh,
        in_specs=placed,
        out_specs=(P("gx", "gy", "gz", None), P(None, "gx", "gy", "gz", None)),
        check_vma=False,
    )
```

```python
import functools
import math

import jax
import jax.numpy as jnp
from jax import lax
from jax.experimental import pallas as pl
from jax.experimental.pallas import tpu as pltpu
from jax.sharding import PartitionSpec as P

SENTINEL = 4.0
PAIR_SCALE = 0.02
EMBED_SCALE = 0.2
FORCE_SCALE = 8.0
FAR = -1.0e6
ROWS = 8
OCTANTS = 8
SPAN = 32


def split(value):
    first = value.astype(jnp.bfloat16).astype(jnp.float32)
    rest = value - first
    second = rest.astype(jnp.bfloat16).astype(jnp.float32)
    return first, second, rest - second


NAMES = ("gx", "gy", "gz")
DIRECTIONS = [
    (x, y, z) for x in (-1, 0, 1) for y in (-1, 0, 1) for z in (-1, 0, 1) if (x, y, z) != (0, 0, 0)
]
DIRECTIONS.sort(key=lambda step: (abs(step[0]) * (1 + abs(step[1])), -sum(map(abs, step))))


def device_at(counts, step):
    return {
        name: lax.rem(lax.axis_index(name) + (offset + count), count)
        for name, offset, count in zip(NAMES, step, counts)
    }


def partners(counts):
    return sorted({tuple(o % c for o, c in zip(step, counts)) for step in DIRECTIONS})


def greet(counts):
    barrier = pltpu.get_barrier_semaphore()
    for step in partners(counts):
        pl.semaphore_signal(
            barrier,
            inc=1,
            device_id=device_at(counts, step),
            device_id_type=pl.DeviceIdType.MESH,
        )


def meet(counts):
    pl.semaphore_wait(pltpu.get_barrier_semaphore(), len(partners(counts)))


def kind_of(step):
    return (2 if step[0] else 0) + (1 if step[1] else 0)


def send_rims(counts, source, target, sent, landed):
    lead = (slice(None),) * (source.ndim - 5)
    sizes = source.shape[-5:-2]
    for step in DIRECTIONS:
        here = tuple(
            pl.ds(0, size) if o == 0 else pl.ds(size - 1 if o > 0 else 0, 1)
            for o, size in zip(step, sizes)
        )
        there = tuple(
            pl.ds(1, size) if o == 0 else pl.ds(0 if o > 0 else size + 1, 1)
            for o, size in zip(step, sizes)
        )
        pltpu.make_async_remote_copy(
            src_ref=source.at[lead + here],
            dst_ref=target.at[lead + there],
            send_sem=sent.at[kind_of(step)],
            recv_sem=landed.at[kind_of(step)],
            device_id=device_at(counts, step),
            device_id_type=pl.DeviceIdType.MESH,
        ).start()


def arrive(kind, target, sizes, sent, landed):
    sx, sy, _ = sizes
    lead = (slice(None),) * (target.ndim - 5)
    extent = ((sx, sy, 2), (sx, 2, sizes[2] + 2), (2, sy, sizes[2] + 2), (2, 2, sizes[2] + 2))[kind]
    whole = target.at[lead + tuple(pl.ds(0, size) for size in extent)]
    pltpu.make_async_copy(whole, whole, sent.at[kind]).wait()
    pltpu.make_async_copy(whole, whole, landed.at[kind]).wait()


def halves(value):
    high = value.astype(jnp.bfloat16)
    return high, (value - high.astype(jnp.float32)).astype(jnp.bfloat16)


def kernel(
    mesh_counts,
    counts,
    positions,
    energy_ref,
    force_ref,
    held,
    raw,
    source,
    ext,
    far,
    gain_own,
    gain_ext,
    order,
    pieces_of,
    picks,
    weights,
    lanes_of,
    dense,
    piles,
    table_rows,
    table,
    fetch_sem,
    table_sem,
    sent,
    landed,
    gain_landed,
):
    sizes = gain_own.shape[:3]
    sx, sy, sz = sizes
    wide = gain_ext.shape[:3]
    wx, wy, wz = wide
    slots = source.shape[-1]
    cells = sx * sy * sz
    group_count = weights.shape[1]
    depth = picks.shape[1]
    plane = wy * wz

    fetches = [
        pltpu.make_async_copy(counts, held, fetch_sem.at[0]),
        pltpu.make_async_copy(positions, raw, fetch_sem.at[1]),
    ]
    for fetch in fetches:
        fetch.start()
    greet(mesh_counts)

    lane = lax.broadcasted_iota(jnp.int32, (cells, slots), 1)
    cell = lax.broadcasted_iota(jnp.int32, (cells, slots), 0)
    column_of = sum(((cell >= k * sz).astype(jnp.int32) for k in range(1, sx * sy)), jnp.zeros_like(cell))
    plane_of = sum(((column_of >= k * sy).astype(jnp.int32) for k in range(1, sx)), jnp.zeros_like(cell))
    spots = (plane_of, column_of - plane_of * sy, cell - column_of * sz)

    for fetch in fetches:
        fetch.wait()
    occupancy = jnp.zeros((cells, slots), jnp.int32)
    for x in range(sx):
        for y in range(sy):
            for z in range(sz):
                occupancy = jnp.where(cell == (x * sy + y) * sz + z, held[x, y, z], occupancy)
    filled = lane < occupancy
    seated = [
        jnp.where(filled, raw[k].reshape(cells, slots), SENTINEL) for k in range(3)
    ]
    for k in range(3):
        source[k] = seated[k].reshape(sizes + (1, slots))

    meet(mesh_counts)
    send_rims(mesh_counts, source, ext, sent, landed)

    own = [
        jnp.where(
            filled,
            seated[k] + ((spots[k] + 1).astype(jnp.float32) - 0.5 * wide[k]),
            0.0,
        )
        for k in range(3)
    ]
    inner = tuple(slice(1, 1 + size) for size in sizes)
    for k in range(3):
        ext[(k,) + inner] = seated[k].reshape(sizes + (1, slots))

    upper = [(seated[k] >= 0.5).astype(jnp.int32) for k in range(3)]
    octant = jnp.where(filled, 4 * upper[0] + 2 * upper[1] + upper[2], OCTANTS)
    members = jnp.concatenate(
        [jnp.where(octant == o, 1.0, 0.0) for o in range(OCTANTS)], axis=0
    ).astype(jnp.bfloat16)
    before = lax.broadcasted_iota(jnp.int32, (slots, 2 * slots), 0)
    after = lax.broadcasted_iota(jnp.int32, (slots, 2 * slots), 1)
    earlier = jnp.where((after >= slots) | (before < after), 1.0, 0.0).astype(jnp.bfloat16)
    ranks = jnp.dot(members, earlier, preferred_element_type=jnp.float32).astype(jnp.int32)
    start = jnp.zeros((cells, slots), jnp.int32)
    place = jnp.full((cells, slots), -1, jnp.int32)
    block = jnp.zeros((cells, slots), jnp.int32)
    phase_of = lane // SPAN
    group = lane - phase_of * SPAN
    for o in range(OCTANTS):
        rows = ranks[o * cells : (o + 1) * cells]
        place = jnp.where(octant == o, start + rows[:, :slots], place)
        if o:
            block = block + jnp.where(group * ROWS >= start, 1, 0)
        start = start + ((rows[:, slots:] + (ROWS - 1)) & -ROWS)
    order[...] = place
    bits = [(block >> 2) & 1, (block >> 1) & 1, block & 1]
    far_x = jnp.where(phase_of >= 2, spots[0] + 2 * bits[0], spots[0] + 1)
    far_y = jnp.where((phase_of & 1) == 1, spots[1] + 2 * bits[1], spots[1] + 1)
    table_rows[...] = (far_x * wy + far_y) * wz + spots[2] + bits[2]
    tabulate = pltpu.make_async_copy(table_rows, table, table_sem)
    tabulate.start()

    near = 1.0 - 4.0 * (own[0] * own[0] + own[1] * own[1] + own[2] * own[2])
    for k, value in enumerate([8.0 * own[0], 8.0 * own[1], 8.0 * own[2], near]):
        for part, piece in enumerate(split(value)):
            pieces_of[part, k] = piece

    batch = next(n for n in (8, 4, 2, 1) if cells % n == 0)
    kind_row = lax.broadcasted_iota(jnp.int32, (16, 4 * slots), 0)
    kind_lane = lax.broadcasted_iota(jnp.int32, (16, 4 * slots), 1)
    smear = jnp.where(
        (kind_row < 12) & ((kind_row & 3) == kind_lane // slots), 1.0, 0.0
    ).astype(jnp.bfloat16)

    def sort_cells(i, carry):
        found = []
        for j in range(batch):
            c = i * batch + j
            spot = order[pl.ds(c, 1), :]
            target = lax.broadcasted_iota(jnp.int32, (depth, slots), 0)
            pick = jnp.where(target == spot, 1.0, 0.0).astype(jnp.bfloat16)
            picks[c] = pick
            rows = [pieces_of[part, k, pl.ds(c, 1), :] for part in range(3) for k in range(4)]
            rows += [jnp.zeros((4, slots), jnp.float32)]
            found.append(
                lax.dot_general(
                    pick,
                    jnp.concatenate(rows, axis=0).astype(jnp.bfloat16),
                    (((1,), (1,)), ((), ())),
                    preferred_element_type=jnp.float32,
                ).astype(jnp.bfloat16)
            )
        for j in range(batch):
            spread = jnp.dot(found[j], smear, preferred_element_type=jnp.float32)
            for k in range(4):
                for g in range(group_count):
                    lanes_of[i * batch + j, g, k] = spread[
                        g * ROWS : (g + 1) * ROWS, k * slots : (k + 1) * slots
                    ]
        return carry

    lax.fori_loop(0, cells // batch, sort_cells, 0)

    def prepare(x, y, z, count):
        shape = (count, 1, slots)
        rows = [ext[k, x, y, pl.ds(z, count)] for k in range(3)]
        there = rows[0] < 2.0
        floor = lax.broadcasted_iota(jnp.int32, shape, 0).astype(jnp.float32) + (z - 0.5 * wz)
        shifts = (
            lax.convert_element_type(x, jnp.float32) - 0.5 * wx,
            lax.convert_element_type(y, jnp.float32) - 0.5 * wy,
            floor,
        )
        coords = [jnp.where(there, row + shift, 0.0) for row, shift in zip(rows, shifts)]
        squares = coords[0] * coords[0] + coords[1] * coords[1] + coords[2] * coords[2]
        at = pl.ds((x * wy + y) * wz + z, count)
        for k in range(3):
            far[at, k : k + 1] = coords[k]
        far[at, 3:4] = jnp.where(there, -4.0 * squares, FAR)

    def prepare_gain(x, y, z, count):
        far[pl.ds((x * wy + y) * wz + z, count), 4:5] = gain_ext[x, y, pl.ds(z, count)]

    def far_row(at, k):
        return jnp.broadcast_to(far[at, k : k + 1], (ROWS, slots))

    def columns(count, where, body):
        def step(i, carry):
            body(*where(i))
            return carry

        lax.fori_loop(0, count, step, 0)

    def inner_columns(body):
        columns(sx * sy, lambda i: (i // sy + 1, i % sy + 1), lambda x, y: body(x, y, 1, sz))

    def end_columns(body):
        def ends(x, y):
            body(x, y, 0, 1)
            body(x, y, wz - 1, 1)

        columns(sx * sy, lambda i: (i // sy + 1, i % sy + 1), ends)

    def plane_columns(body):
        columns(
            2 * sx, lambda i: (i // 2 + 1, i % 2 * (wy - 1)), lambda x, y: body(x, y, 0, wz)
        )

    def side_columns(ys, count, body):
        columns(
            2 * count,
            lambda i: (i // count * (wx - 1), ys(i % count)),
            lambda x, y: body(x, y, 0, wz),
        )

    def face_columns(body):
        side_columns(lambda y: y + 1, sy, body)

    def edge_columns(body):
        side_columns(lambda y: y * (wy - 1), 2, body)

    slot_lane = lax.broadcasted_iota(jnp.int32, (ROWS, slots), 1)

    def lane_sums(c, rows, parts):
        kept = dense[rows, :]
        for k, part in enumerate(parts):
            kept = jnp.where(
                slot_lane == k * cells + c, jnp.sum(part, axis=1, keepdims=True), kept
            )
        dense[rows, :] = kept

    def sorted_rows(kinds):
        flat = dense[...].T
        return [flat[k * cells : (k + 1) * cells, :depth] for k in range(kinds)]

    def batched(count, most, where, body, phases):
        several = next(n for n in range(most, 0, -1) if count % n == 0)

        def step(i, carry):
            for j in range(several):
                body(where(i * several + j), phases)
            return carry

        lax.fori_loop(0, count // several, step, 0)

    def all_cells(body, *phases):
        batched(cells, 2, lambda i: i, body, phases)

    def last_cells(body, *phases):
        batched(cells, 4, lambda i: i, body, phases)

    def middle_cells(body):
        span = sz - 2
        if span > 0:
            batched(sx * sy * span, 2, lambda i: i // span * sz + 1 + i % span, body, (0,))

    def end_cells(body):
        ends = min(sz, 2)
        columns(
            ends * sx * sy,
            lambda i: (i // ends * sz + i % ends * (sz - 1),),
            lambda c: body(c, (0,)),
        )

    def density(c, phases):
        def one_group(g, inside):
            xi, yi, zi, ci = (lanes_of[c, g, k] for k in range(4))
            if phases[0]:
                rho, quartic = lanes_of[c, g, 4], lanes_of[c, g, 5]
            else:
                rho, quartic = (jnp.zeros((ROWS, slots), jnp.float32),) * 2
            for phase in phases:
                base = table[c, phase * SPAN + g]
                for step in range(2):
                    at = base + step
                    t = (far_row(at, 3) + ci) + xi * far_row(at, 0)
                    t = t + yi * far_row(at, 1) + zi * far_row(at, 2)
                    w = jnp.maximum(t, 0.0)
                    weights[c, g, 2 * phase + step] = w
                    s = w * w
                    rho = rho + s
                    quartic = quartic + s * s
            if phases[-1] == 3:
                lane_sums(c, pl.ds(g * ROWS, ROWS), (rho, quartic))
            else:
                lanes_of[c, g, 4] = rho
                lanes_of[c, g, 5] = quartic
            return inside

        lax.fori_loop(0, group_count, one_group, 0, unroll=True)

    def force(c, phases):
        def one_group(g, inside):
            gi = lanes_of[c, g, 3]
            if phases[0]:
                parts = [lanes_of[c, g, 4 + k] for k in range(4)]
            else:
                parts = [jnp.zeros((ROWS, slots), jnp.float32)] * 4
            for phase in phases:
                base = table[c, phase * SPAN + g]
                for step in range(2):
                    at = base + step
                    w = weights[c, g, 2 * phase + step]
                    f = w * ((far_row(at, 4) + gi) - w * w)
                    for k in range(3):
                        parts[k] = parts[k] + f * far_row(at, k)
                    parts[3] = parts[3] + f
            if phases[-1] == 3:
                whole = 0.125 * parts[3]
                parts = [parts[k] - lanes_of[c, g, k] * whole for k in range(3)]
                lane_sums(c, pl.ds(g * ROWS, ROWS), parts)
            else:
                for k in range(4):
                    lanes_of[c, g, 4 + k] = parts[k]
            return inside

        lax.fori_loop(0, group_count, one_group, 0, unroll=True)

    def unsort(kinds):
        pieces = [piece for value in kinds for piece in halves(value)]
        pieces = jnp.concatenate(pieces, axis=0)
        tall = pieces.shape[0]
        row = lax.broadcasted_iota(jnp.int32, pieces.shape, 0) % cells
        for lot in range(lots):
            total = jnp.zeros((tall, pair * slots), jnp.float32)
            for c in range(lot * cells // lots, (lot + 1) * cells // lots, pair):
                kept = jnp.where((row >= c) & (row < c + pair), pieces, jnp.zeros_like(pieces))
                both = jnp.concatenate([picks[c + j] for j in range(pair)], axis=1)
                total = total + jnp.dot(kept, both, preferred_element_type=jnp.float32)
            piles[lot, :tall] = total
        total = sum(piles[lot, :tall] for lot in range(lots))
        odd = lax.broadcasted_iota(jnp.int32, (tall, slots), 0) % pair
        total = functools.reduce(
            lambda kept, j: jnp.where(odd == j, total[:, j * slots : (j + 1) * slots], kept),
            range(1, pair),
            total[:, :slots],
        )
        rows = [total[k * cells : (k + 1) * cells] for k in range(2 * len(kinds))]
        return [rows[2 * k] + rows[2 * k + 1] for k in range(len(kinds))]

    pair = 2 if cells % 2 == 0 else 1
    lots = 2 if cells % 4 == 0 else 1

    def land(kind):
        arrive(kind, ext, sizes, sent, landed)

    def land_gain(kind):
        arrive(kind, gain_ext, sizes, sent, gain_landed)

    dense[...] = jnp.zeros_like(dense)
    inner_columns(prepare)
    tabulate.wait()
    middle_cells(density)
    land(0)
    end_columns(prepare)
    end_cells(density)
    land(1)
    plane_columns(prepare)
    all_cells(density, 1)
    land(2)
    face_columns(prepare)
    all_cells(density, 2)
    land(3)
    edge_columns(prepare)
    last_cells(density, 3)

    rho_rows, quartic_rows = sorted_rows(2)
    first = jnp.maximum(rho_rows - 1.0, 0.0)
    second = jnp.maximum(quartic_rows - 1.0, 0.0)
    fprime = -0.5 * EMBED_SCALE * lax.rsqrt(first + 1.0)
    gain = 0.5 - fprime * (0.5 / PAIR_SCALE)
    gain_rows = unsort([gain])[0]
    gain_own[...] = gain_rows.reshape(sizes + (1, slots))
    send_rims(mesh_counts, gain_own, gain_ext, sent, gain_landed)
    gain_ext[inner] = gain_rows.reshape(sizes + (1, slots))
    pair_sum = PAIR_SCALE * (second - 2.0 * first)
    energy = -EMBED_SCALE * jnp.sqrt(first + 1.0) + 0.5 * pair_sum
    energy_rows = unsort([energy])[0]
    energy_ref[...] = jnp.where(filled, energy_rows, 0.0).reshape(sizes + (slots,))

    tall = [piece.astype(jnp.float32) for piece in halves(gain)]
    tall += [jnp.zeros((slots - 2 * cells, depth), jnp.float32)]
    tall = jnp.concatenate(tall, axis=0)
    tall = jnp.concatenate([tall, jnp.zeros((slots, -depth % 128), jnp.float32)], axis=1)
    standing = tall.T[:depth].astype(jnp.bfloat16)
    pick_row = lax.broadcasted_iota(jnp.int32, (slots, pair * slots), 0)
    pick_cell = jnp.where(
        pick_row < 2 * cells, pick_row - jnp.where(pick_row >= cells, cells, 0), -1
    )
    pick_lane = lax.broadcasted_iota(jnp.int32, (slots, pair * slots), 1) // slots
    for i in range(cells // pair):
        chosen = jnp.where(pick_cell == pair * i + pick_lane, 1.0, 0.0).astype(jnp.bfloat16)
        spread = jnp.dot(standing, chosen, preferred_element_type=jnp.float32)
        for j in range(pair):
            for g in range(group_count):
                lanes_of[pair * i + j, g, 3] = spread[
                    g * ROWS : (g + 1) * ROWS, j * slots : (j + 1) * slots
                ]

    inner_columns(prepare_gain)
    middle_cells(force)
    land_gain(0)
    end_columns(prepare_gain)
    end_cells(force)
    land_gain(1)
    plane_columns(prepare_gain)
    all_cells(force, 1)
    land_gain(2)
    face_columns(prepare_gain)
    land_gain(3)
    edge_columns(prepare_gain)
    last_cells(force, 2, 3)

    scale = FORCE_SCALE * 4.0 * PAIR_SCALE
    pushes = unsort(sorted_rows(3))
    for k, push in enumerate(pushes):
        force_ref[k] = jnp.where(filled, scale * push, 0.0).reshape(sizes + (slots,))


def per_device(mesh_counts, positions, counts):
    slots = positions.shape[-1]
    sizes = positions.shape[1:4]
    wide = tuple(size + 2 for size in sizes)
    cells = sizes[0] * sizes[1] * sizes[2]
    far_cells = wide[0] * wide[1] * wide[2]
    groups = (slots + OCTANTS * (ROWS - 1)) // ROWS
    depth = -(-groups // 2) * 2 * ROWS
    f32, bf16, i32 = jnp.float32, jnp.bfloat16, jnp.int32
    vmem = [
        ((3,) + sizes + (slots,), f32),
        ((3,) + sizes + (1, slots), f32),
        ((3,) + wide + (1, slots), f32),
        ((far_cells, ROWS, slots), f32),
        (sizes + (1, slots), f32),
        (wide + (1, slots), f32),
        ((cells, slots), i32),
        ((3, 4, cells, slots), f32),
        ((cells, depth, slots), bf16),
        ((cells, groups, 8, ROWS, slots), f32),
        ((cells, groups, 8, ROWS, slots), f32),
        ((-(-depth // 128) * 128, slots), f32),
        ((2, 6 * cells, 2 * slots), f32),
        ((cells, slots), i32),
    ]
    held = sum(math.prod(shape) * jnp.dtype(kind).itemsize for shape, kind in vmem)
    return pl.pallas_call(
        functools.partial(kernel, mesh_counts),
        out_shape=(
            jax.ShapeDtypeStruct(sizes + (slots,), f32),
            jax.ShapeDtypeStruct((3,) + sizes + (slots,), f32),
        ),
        in_specs=[pl.BlockSpec(memory_space=pltpu.HBM)] * 2,
        out_specs=(pl.BlockSpec(memory_space=pltpu.VMEM),) * 2,
        scratch_shapes=[pltpu.SMEM(counts.shape, i32)]
        + [pltpu.VMEM(shape, kind) for shape, kind in vmem]
        + [
            pltpu.SMEM((cells, slots), i32),
            pltpu.SemaphoreType.DMA((2,)),
            pltpu.SemaphoreType.DMA,
        ]
        + [pltpu.SemaphoreType.DMA((4,))] * 3,
        compiler_params=pltpu.CompilerParams(
            collective_id=0,
            has_side_effects=True,
            vmem_limit_bytes=held + (4 << 20),
        ),
        name="atoms",
    )(*(pltpu.with_memory_space_constraint(x, pltpu.HBM) for x in (counts, positions)))


def solution(mesh):
    placed = (P(None, "gx", "gy", "gz", None), P("gx", "gy", "gz"))
    return jax.shard_map(
        functools.partial(per_device, tuple(mesh.shape[name] for name in NAMES)),
        mesh=mesh,
        in_specs=placed,
        out_specs=(P("gx", "gy", "gz", None), P(None, "gx", "gy", "gz", None)),
        check_vma=False,
    )
```

```python
import functools
import math

import jax
import jax.numpy as jnp
from jax import lax
from jax.experimental import pallas as pl
from jax.experimental.pallas import tpu as pltpu
from jax.sharding import PartitionSpec as P

SENTINEL = 4.0
PAIR_SCALE = 0.02
EMBED_SCALE = 0.2
FORCE_SCALE = 8.0
FAR = -1.0e6
ROWS = 8
OCTANTS = 8
SPAN = 32


def split(value):
    first = value.astype(jnp.bfloat16).astype(jnp.float32)
    rest = value - first
    second = rest.astype(jnp.bfloat16).astype(jnp.float32)
    return first, second, rest - second


NAMES = ("gx", "gy", "gz")
DIRECTIONS = [
    (x, y, z) for x in (-1, 0, 1) for y in (-1, 0, 1) for z in (-1, 0, 1) if (x, y, z) != (0, 0, 0)
]
DIRECTIONS.sort(key=lambda step: (abs(step[0]) * (1 + abs(step[1])), -sum(map(abs, step))))


def device_at(counts, step):
    return {
        name: lax.rem(lax.axis_index(name) + (offset + count), count)
        for name, offset, count in zip(NAMES, step, counts)
    }


def partners(counts):
    return sorted(
        {tuple(o % c for o, c in zip(step, counts)) for step in DIRECTIONS},
        key=lambda step: [-min(o, c - o) for o, c in zip(step, counts)],
    )


def greet(counts):
    barrier = pltpu.get_barrier_semaphore()
    for step in partners(counts):
        pl.semaphore_signal(
            barrier,
            inc=1,
            device_id=device_at(counts, step),
            device_id_type=pl.DeviceIdType.MESH,
        )


def meet(counts):
    pl.semaphore_wait(pltpu.get_barrier_semaphore(), len(partners(counts)))


def kind_of(step):
    return (2 if step[0] else 0) + (1 if step[1] else 0)


def send_rims(counts, source, target, sent, landed):
    lead = (slice(None),) * (source.ndim - 5)
    sizes = source.shape[-5:-2]
    for step in DIRECTIONS:
        here = tuple(
            pl.ds(0, size) if o == 0 else pl.ds(size - 1 if o > 0 else 0, 1)
            for o, size in zip(step, sizes)
        )
        there = tuple(
            pl.ds(1, size) if o == 0 else pl.ds(0 if o > 0 else size + 1, 1)
            for o, size in zip(step, sizes)
        )
        pltpu.make_async_remote_copy(
            src_ref=source.at[lead + here],
            dst_ref=target.at[lead + there],
            send_sem=sent.at[kind_of(step)],
            recv_sem=landed.at[kind_of(step)],
            device_id=device_at(counts, step),
            device_id_type=pl.DeviceIdType.MESH,
        ).start()


def arrive(kind, target, sizes, sent, landed):
    sx, sy, _ = sizes
    lead = (slice(None),) * (target.ndim - 5)
    extent = ((sx, sy, 2), (sx, 2, sizes[2] + 2), (2, sy, sizes[2] + 2), (2, 2, sizes[2] + 2))[kind]
    whole = target.at[lead + tuple(pl.ds(0, size) for size in extent)]
    pltpu.make_async_copy(whole, whole, sent.at[kind]).wait()
    pltpu.make_async_copy(whole, whole, landed.at[kind]).wait()


def halves(value):
    high = value.astype(jnp.bfloat16)
    return high, (value - high.astype(jnp.float32)).astype(jnp.bfloat16)


def kernel(
    mesh_counts,
    counts,
    positions,
    energy_ref,
    force_ref,
    held,
    raw,
    source,
    ext,
    far,
    gain_own,
    gain_ext,
    order,
    pieces_of,
    picks,
    weights,
    lanes_of,
    dense,
    piles,
    table_rows,
    table,
    fetch_sem,
    table_sem,
    sent,
    landed,
    gain_landed,
):
    sizes = gain_own.shape[:3]
    sx, sy, sz = sizes
    wide = gain_ext.shape[:3]
    wx, wy, wz = wide
    slots = source.shape[-1]
    cells = sx * sy * sz
    group_count = weights.shape[1]
    depth = picks.shape[1]
    plane = wy * wz

    fetches = [
        pltpu.make_async_copy(counts, held, fetch_sem.at[0]),
        pltpu.make_async_copy(positions, raw, fetch_sem.at[1]),
    ]
    for fetch in fetches:
        fetch.start()
    greet(mesh_counts)

    lane = lax.broadcasted_iota(jnp.int32, (cells, slots), 1)
    cell = lax.broadcasted_iota(jnp.int32, (cells, slots), 0)
    column_of = sum(((cell >= k * sz).astype(jnp.int32) for k in range(1, sx * sy)), jnp.zeros_like(cell))
    plane_of = sum(((column_of >= k * sy).astype(jnp.int32) for k in range(1, sx)), jnp.zeros_like(cell))
    spots = (plane_of, column_of - plane_of * sy, cell - column_of * sz)

    for fetch in fetches:
        fetch.wait()
    occupancy = jnp.zeros((cells, slots), jnp.int32)
    for x in range(sx):
        for y in range(sy):
            for z in range(sz):
                occupancy = jnp.where(cell == (x * sy + y) * sz + z, held[x, y, z], occupancy)
    filled = lane < occupancy
    seated = [
        jnp.where(filled, raw[k].reshape(cells, slots), SENTINEL) for k in range(3)
    ]
    for k in range(3):
        source[k] = seated[k].reshape(sizes + (1, slots))


    own = [
        jnp.where(
            filled,
            seated[k] + ((spots[k] + 1).astype(jnp.float32) - 0.5 * wide[k]),
            0.0,
        )
        for k in range(3)
    ]
    inner = tuple(slice(1, 1 + size) for size in sizes)
    for k in range(3):
        ext[(k,) + inner] = seated[k].reshape(sizes + (1, slots))

    upper = [(seated[k] >= 0.5).astype(jnp.int32) for k in range(3)]
    octant = jnp.where(filled, 4 * upper[0] + 2 * upper[1] + upper[2], OCTANTS)
    members = jnp.concatenate(
        [jnp.where(octant == o, 1.0, 0.0) for o in range(OCTANTS)], axis=0
    ).astype(jnp.bfloat16)
    before = lax.broadcasted_iota(jnp.int32, (slots, 2 * slots), 0)
    after = lax.broadcasted_iota(jnp.int32, (slots, 2 * slots), 1)
    earlier = jnp.where((after >= slots) | (before < after), 1.0, 0.0).astype(jnp.bfloat16)
    ranks = jnp.dot(members, earlier, preferred_element_type=jnp.float32).astype(jnp.int32)
    start = jnp.zeros((cells, slots), jnp.int32)
    place = jnp.full((cells, slots), -1, jnp.int32)
    block = jnp.zeros((cells, slots), jnp.int32)
    phase_of = lane // SPAN
    group = lane - phase_of * SPAN
    for o in range(OCTANTS):
        rows = ranks[o * cells : (o + 1) * cells]
        place = jnp.where(octant == o, start + rows[:, :slots], place)
        if o:
            block = block + jnp.where(group * ROWS >= start, 1, 0)
        start = start + ((rows[:, slots:] + (ROWS - 1)) & -ROWS)
    order[...] = place
    bits = [(block >> 2) & 1, (block >> 1) & 1, block & 1]
    far_x = jnp.where(phase_of >= 2, spots[0] + 2 * bits[0], spots[0] + 1)
    far_y = jnp.where((phase_of & 1) == 1, spots[1] + 2 * bits[1], spots[1] + 1)
    table_rows[...] = (far_x * wy + far_y) * wz + spots[2] + bits[2]
    tabulate = pltpu.make_async_copy(table_rows, table, table_sem)
    tabulate.start()

    near = 1.0 - 4.0 * (own[0] * own[0] + own[1] * own[1] + own[2] * own[2])
    for k, value in enumerate([8.0 * own[0], 8.0 * own[1], 8.0 * own[2], near]):
        for part, piece in enumerate(split(value)):
            pieces_of[part, k] = piece

    batch = next(n for n in (8, 4, 2, 1) if cells % n == 0)
    kind_row = lax.broadcasted_iota(jnp.int32, (16, 4 * slots), 0)
    kind_lane = lax.broadcasted_iota(jnp.int32, (16, 4 * slots), 1)
    smear = jnp.where(
        (kind_row < 12) & ((kind_row & 3) == kind_lane // slots), 1.0, 0.0
    ).astype(jnp.bfloat16)

    def sort_cells(i, carry):
        found = []
        for j in range(batch):
            c = i * batch + j
            spot = order[pl.ds(c, 1), :]
            target = lax.broadcasted_iota(jnp.int32, (depth, slots), 0)
            pick = jnp.where(target == spot, 1.0, 0.0).astype(jnp.bfloat16)
            picks[c] = pick
            rows = [pieces_of[part, k, pl.ds(c, 1), :] for part in range(3) for k in range(4)]
            rows += [jnp.zeros((4, slots), jnp.float32)]
            found.append(
                lax.dot_general(
                    pick,
                    jnp.concatenate(rows, axis=0).astype(jnp.bfloat16),
                    (((1,), (1,)), ((), ())),
                    preferred_element_type=jnp.float32,
                ).astype(jnp.bfloat16)
            )
        for j in range(batch):
            spread = jnp.dot(found[j], smear, preferred_element_type=jnp.float32)
            for k in range(4):
                for g in range(group_count):
                    lanes_of[i * batch + j, g, k] = spread[
                        g * ROWS : (g + 1) * ROWS, k * slots : (k + 1) * slots
                    ]
        return carry

    lax.fori_loop(0, cells // batch, sort_cells, 0)
    meet(mesh_counts)
    send_rims(mesh_counts, source, ext, sent, landed)

    def prepare(x, y, z, count):
        shape = (count, 1, slots)
        rows = [ext[k, x, y, pl.ds(z, count)] for k in range(3)]
        there = rows[0] < 2.0
        floor = lax.broadcasted_iota(jnp.int32, shape, 0).astype(jnp.float32) + (z - 0.5 * wz)
        shifts = (
            lax.convert_element_type(x, jnp.float32) - 0.5 * wx,
            lax.convert_element_type(y, jnp.float32) - 0.5 * wy,
            floor,
        )
        coords = [jnp.where(there, row + shift, 0.0) for row, shift in zip(rows, shifts)]
        squares = coords[0] * coords[0] + coords[1] * coords[1] + coords[2] * coords[2]
        at = pl.ds((x * wy + y) * wz + z, count)
        for k in range(3):
            far[at, k : k + 1] = coords[k]
        far[at, 3:4] = jnp.where(there, -4.0 * squares, FAR)

    def prepare_gain(x, y, z, count):
        far[pl.ds((x * wy + y) * wz + z, count), 4:5] = gain_ext[x, y, pl.ds(z, count)]

    def far_row(at, k):
        return jnp.broadcast_to(far[at, k : k + 1], (ROWS, slots))

    def columns(count, where, body):
        def step(i, carry):
            body(*where(i))
            return carry

        lax.fori_loop(0, count, step, 0)

    def inner_columns(body):
        columns(sx * sy, lambda i: (i // sy + 1, i % sy + 1), lambda x, y: body(x, y, 1, sz))

    def end_columns(body):
        def ends(x, y):
            body(x, y, 0, 1)
            body(x, y, wz - 1, 1)

        columns(sx * sy, lambda i: (i // sy + 1, i % sy + 1), ends)

    def plane_columns(body):
        columns(
            2 * sx, lambda i: (i // 2 + 1, i % 2 * (wy - 1)), lambda x, y: body(x, y, 0, wz)
        )

    def side_columns(ys, count, body):
        columns(
            2 * count,
            lambda i: (i // count * (wx - 1), ys(i % count)),
            lambda x, y: body(x, y, 0, wz),
        )

    def face_columns(body):
        side_columns(lambda y: y + 1, sy, body)

    def edge_columns(body):
        side_columns(lambda y: y * (wy - 1), 2, body)

    slot_lane = lax.broadcasted_iota(jnp.int32, (ROWS, slots), 1)

    def lane_sums(c, rows, parts):
        kept = dense[rows, :]
        for k, part in enumerate(parts):
            kept = jnp.where(
                slot_lane == k * cells + c, jnp.sum(part, axis=1, keepdims=True), kept
            )
        dense[rows, :] = kept

    def sorted_rows(kinds):
        flat = dense[...].T
        return [flat[k * cells : (k + 1) * cells, :depth] for k in range(kinds)]

    def batched(count, most, where, body, phases):
        several = next(n for n in range(most, 0, -1) if count % n == 0)

        def step(i, carry):
            for j in range(several):
                body(where(i * several + j), phases)
            return carry

        lax.fori_loop(0, count // several, step, 0)

    def all_cells(body, *phases):
        batched(cells, 4, lambda i: i, body, phases)

    def last_cells(body, *phases):
        batched(cells, 8, lambda i: i, body, phases)

    def middle_cells(body):
        span = sz - 2
        if span > 0:
            batched(sx * sy * span, 2, lambda i: i // span * sz + 1 + i % span, body, (0,))

    def end_cells(body):
        ends = min(sz, 2)
        columns(
            ends * sx * sy,
            lambda i: (i // ends * sz + i % ends * (sz - 1),),
            lambda c: body(c, (0,)),
        )

    def density(c, phases):
        def one_group(g, inside):
            xi, yi, zi, ci = (lanes_of[c, g, k] for k in range(4))
            if phases[0]:
                rho, quartic = lanes_of[c, g, 4], lanes_of[c, g, 5]
            else:
                rho, quartic = (jnp.zeros((ROWS, slots), jnp.float32),) * 2
            for phase in phases:
                base = table[c, phase * SPAN + g]
                for step in range(2):
                    at = base + step
                    t = (far_row(at, 3) + ci) + xi * far_row(at, 0)
                    t = t + yi * far_row(at, 1) + zi * far_row(at, 2)
                    w = jnp.maximum(t, 0.0)
                    weights[c, g, 2 * phase + step] = w
                    s = w * w
                    rho = rho + s
                    quartic = quartic + s * s
            if phases[-1] == 3:
                lane_sums(c, pl.ds(g * ROWS, ROWS), (rho, quartic))
            else:
                lanes_of[c, g, 4] = rho
                lanes_of[c, g, 5] = quartic
            return inside

        lax.fori_loop(0, group_count, one_group, 0, unroll=True)

    def force(c, phases):
        def one_group(g, inside):
            gi = lanes_of[c, g, 3]
            if phases[0]:
                parts = [lanes_of[c, g, 4 + k] for k in range(4)]
            else:
                parts = [jnp.zeros((ROWS, slots), jnp.float32)] * 4
            for phase in phases:
                base = table[c, phase * SPAN + g]
                for step in range(2):
                    at = base + step
                    w = weights[c, g, 2 * phase + step]
                    f = w * ((far_row(at, 4) + gi) - w * w)
                    for k in range(3):
                        parts[k] = parts[k] + f * far_row(at, k)
                    parts[3] = parts[3] + f
            if phases[-1] == 3:
                whole = 0.125 * parts[3]
                parts = [parts[k] - lanes_of[c, g, k] * whole for k in range(3)]
                lane_sums(c, pl.ds(g * ROWS, ROWS), parts)
            else:
                for k in range(4):
                    lanes_of[c, g, 4 + k] = parts[k]
            return inside

        lax.fori_loop(0, group_count, one_group, 0, unroll=True)

    def unsort(kinds):
        pieces = [piece for value in kinds for piece in halves(value)]
        pieces = jnp.concatenate(pieces, axis=0)
        tall = pieces.shape[0]
        row = lax.broadcasted_iota(jnp.int32, pieces.shape, 0) % cells
        for lot in range(lots):
            total = jnp.zeros((tall, pair * slots), jnp.float32)
            for c in range(lot * cells // lots, (lot + 1) * cells // lots, pair):
                kept = jnp.where((row >= c) & (row < c + pair), pieces, jnp.zeros_like(pieces))
                both = jnp.concatenate([picks[c + j] for j in range(pair)], axis=1)
                total = total + jnp.dot(kept, both, preferred_element_type=jnp.float32)
            piles[lot, :tall] = total
        total = sum(piles[lot, :tall] for lot in range(lots))
        odd = lax.broadcasted_iota(jnp.int32, (tall, slots), 0) % pair
        total = functools.reduce(
            lambda kept, j: jnp.where(odd == j, total[:, j * slots : (j + 1) * slots], kept),
            range(1, pair),
            total[:, :slots],
        )
        rows = [total[k * cells : (k + 1) * cells] for k in range(2 * len(kinds))]
        return [rows[2 * k] + rows[2 * k + 1] for k in range(len(kinds))]

    pair = 2 if cells % 2 == 0 else 1
    lots = 2 if cells % 4 == 0 else 1

    def land(kind):
        arrive(kind, ext, sizes, sent, landed)

    def land_gain(kind):
        arrive(kind, gain_ext, sizes, sent, gain_landed)

    dense[...] = jnp.zeros_like(dense)
    inner_columns(prepare)
    tabulate.wait()
    middle_cells(density)
    land(0)
    end_columns(prepare)
    end_cells(density)
    land(1)
    plane_columns(prepare)
    all_cells(density, 1)
    land(2)
    face_columns(prepare)
    all_cells(density, 2)
    land(3)
    edge_columns(prepare)
    last_cells(density, 3)

    rho_rows, quartic_rows = sorted_rows(2)
    first = jnp.maximum(rho_rows - 1.0, 0.0)
    second = jnp.maximum(quartic_rows - 1.0, 0.0)
    fprime = -0.5 * EMBED_SCALE * lax.rsqrt(first + 1.0)
    gain = 0.5 - fprime * (0.5 / PAIR_SCALE)
    gain_rows = unsort([gain])[0]
    gain_own[...] = gain_rows.reshape(sizes + (1, slots))
    send_rims(mesh_counts, gain_own, gain_ext, sent, gain_landed)
    gain_ext[inner] = gain_rows.reshape(sizes + (1, slots))
    pair_sum = PAIR_SCALE * (second - 2.0 * first)
    energy = -EMBED_SCALE * jnp.sqrt(first + 1.0) + 0.5 * pair_sum
    energy_rows = unsort([energy])[0]
    energy_ref[...] = jnp.where(filled, energy_rows, 0.0).reshape(sizes + (slots,))

    tall = [piece.astype(jnp.float32) for piece in halves(gain)]
    tall += [jnp.zeros((slots - 2 * cells, depth), jnp.float32)]
    tall = jnp.concatenate(tall, axis=0)
    tall = jnp.concatenate([tall, jnp.zeros((slots, -depth % 128), jnp.float32)], axis=1)
    standing = tall.T[:depth].astype(jnp.bfloat16)
    pick_row = lax.broadcasted_iota(jnp.int32, (slots, pair * slots), 0)
    pick_cell = jnp.where(
        pick_row < 2 * cells, pick_row - jnp.where(pick_row >= cells, cells, 0), -1
    )
    pick_lane = lax.broadcasted_iota(jnp.int32, (slots, pair * slots), 1) // slots
    for i in range(cells // pair):
        chosen = jnp.where(pick_cell == pair * i + pick_lane, 1.0, 0.0).astype(jnp.bfloat16)
        spread = jnp.dot(standing, chosen, preferred_element_type=jnp.float32)
        for j in range(pair):
            for g in range(group_count):
                lanes_of[pair * i + j, g, 3] = spread[
                    g * ROWS : (g + 1) * ROWS, j * slots : (j + 1) * slots
                ]

    inner_columns(prepare_gain)
    middle_cells(force)
    land_gain(0)
    end_columns(prepare_gain)
    end_cells(force)
    land_gain(1)
    plane_columns(prepare_gain)
    all_cells(force, 1)
    land_gain(2)
    face_columns(prepare_gain)
    land_gain(3)
    edge_columns(prepare_gain)
    last_cells(force, 2, 3)

    scale = FORCE_SCALE * 4.0 * PAIR_SCALE
    pushes = unsort(sorted_rows(3))
    for k, push in enumerate(pushes):
        force_ref[k] = jnp.where(filled, scale * push, 0.0).reshape(sizes + (slots,))


def hand_over(energy, force, energy_out, force_out, done):
    copies = [
        pltpu.make_async_copy(force, force_out, done.at[0]),
        pltpu.make_async_copy(energy, energy_out, done.at[1]),
    ]
    for copy in copies:
        copy.start()
    for copy in copies:
        copy.wait()


def per_device(mesh_counts, positions, counts):
    slots = positions.shape[-1]
    sizes = positions.shape[1:4]
    wide = tuple(size + 2 for size in sizes)
    cells = sizes[0] * sizes[1] * sizes[2]
    far_cells = wide[0] * wide[1] * wide[2]
    groups = (slots + OCTANTS * (ROWS - 1)) // ROWS
    depth = -(-groups // 2) * 2 * ROWS
    f32, bf16, i32 = jnp.float32, jnp.bfloat16, jnp.int32
    vmem = [
        ((3,) + sizes + (slots,), f32),
        ((3,) + sizes + (1, slots), f32),
        ((3,) + wide + (1, slots), f32),
        ((far_cells, ROWS, slots), f32),
        (sizes + (1, slots), f32),
        (wide + (1, slots), f32),
        ((cells, slots), i32),
        ((3, 4, cells, slots), f32),
        ((cells, depth, slots), bf16),
        ((cells, groups, 8, ROWS, slots), f32),
        ((cells, groups, 8, ROWS, slots), f32),
        ((-(-depth // 128) * 128, slots), f32),
        ((2, 6 * cells, 2 * slots), f32),
        ((cells, slots), i32),
    ]
    held = sum(math.prod(shape) * jnp.dtype(kind).itemsize for shape, kind in vmem)
    results = pl.pallas_call(
        functools.partial(kernel, mesh_counts),
        out_shape=(
            jax.ShapeDtypeStruct(sizes + (slots,), f32),
            jax.ShapeDtypeStruct((3,) + sizes + (slots,), f32),
        ),
        in_specs=[pl.BlockSpec(memory_space=pltpu.HBM)] * 2,
        out_specs=(pl.BlockSpec(memory_space=pltpu.VMEM),) * 2,
        scratch_shapes=[pltpu.SMEM(counts.shape, i32)]
        + [pltpu.VMEM(shape, kind) for shape, kind in vmem]
        + [
            pltpu.SMEM((cells, slots), i32),
            pltpu.SemaphoreType.DMA((2,)),
            pltpu.SemaphoreType.DMA,
        ]
        + [pltpu.SemaphoreType.DMA((4,))] * 3,
        compiler_params=pltpu.CompilerParams(
            collective_id=0,
            has_side_effects=True,
            vmem_limit_bytes=held + (4 << 20),
        ),
        name="atoms",
    )(*(pltpu.with_memory_space_constraint(x, pltpu.HBM) for x in (counts, positions)))
    return pl.pallas_call(
        hand_over,
        out_shape=tuple(jax.ShapeDtypeStruct(x.shape, x.dtype) for x in results),
        in_specs=[pl.BlockSpec(memory_space=pltpu.VMEM)] * 2,
        out_specs=(pl.BlockSpec(memory_space=pl.ANY),) * 2,
        scratch_shapes=[pltpu.SemaphoreType.DMA((2,))],
        compiler_params=pltpu.CompilerParams(vmem_limit_bytes=1 << 20),
        name="hand",
    )(*results)


def solution(mesh):
    placed = (P(None, "gx", "gy", "gz", None), P("gx", "gy", "gz"))
    return jax.shard_map(
        functools.partial(per_device, tuple(mesh.shape[name] for name in NAMES)),
        mesh=mesh,
        in_specs=placed,
        out_specs=(P("gx", "gy", "gz", None), P(None, "gx", "gy", "gz", None)),
        check_vma=False,
    )
```

```python
import functools
import math

import jax
import jax.numpy as jnp
from jax import lax
from jax.experimental import pallas as pl
from jax.experimental.pallas import tpu as pltpu
from jax.sharding import PartitionSpec as P

SENTINEL = 4.0
PAIR_SCALE = 0.02
EMBED_SCALE = 0.2
FORCE_SCALE = 8.0
FAR = -1.0e6
ROWS = 8
OCTANTS = 8
SPAN = 32
SLOTS = 8


def split(value):
    first = value.astype(jnp.bfloat16).astype(jnp.float32)
    rest = value - first
    second = rest.astype(jnp.bfloat16).astype(jnp.float32)
    return first, second, rest - second


NAMES = ("gx", "gy", "gz")
DIRECTIONS = [
    (x, y, z) for x in (-1, 0, 1) for y in (-1, 0, 1) for z in (-1, 0, 1) if (x, y, z) != (0, 0, 0)
]
DIRECTIONS.sort(key=lambda step: (abs(step[0]) * (1 + abs(step[1])), -sum(map(abs, step))))


def device_at(counts, step):
    return {
        name: lax.rem(lax.axis_index(name) + (offset + count), count)
        for name, offset, count in zip(NAMES, step, counts)
    }


def partners(counts):
    return sorted(
        {tuple(o % c for o, c in zip(step, counts)) for step in DIRECTIONS},
        key=lambda step: [-min(o, c - o) for o, c in zip(step, counts)],
    )


def greet(counts):
    barrier = pltpu.get_barrier_semaphore()
    for step in partners(counts):
        pl.semaphore_signal(
            barrier,
            inc=1,
            device_id=device_at(counts, step),
            device_id_type=pl.DeviceIdType.MESH,
        )


def meet(counts):
    pl.semaphore_wait(pltpu.get_barrier_semaphore(), len(partners(counts)))


def kind_of(step):
    return (2 if step[0] else 0) + (1 if step[1] else 0)


def send_rims(counts, source, target, sent, landed):
    lead = (slice(None),) * (source.ndim - 5)
    sizes = source.shape[-5:-2]
    for step in DIRECTIONS:
        here = tuple(
            pl.ds(0, size) if o == 0 else pl.ds(size - 1 if o > 0 else 0, 1)
            for o, size in zip(step, sizes)
        )
        there = tuple(
            pl.ds(1, size) if o == 0 else pl.ds(0 if o > 0 else size + 1, 1)
            for o, size in zip(step, sizes)
        )
        pltpu.make_async_remote_copy(
            src_ref=source.at[lead + here],
            dst_ref=target.at[lead + there],
            send_sem=sent.at[kind_of(step)],
            recv_sem=landed.at[kind_of(step)],
            device_id=device_at(counts, step),
            device_id_type=pl.DeviceIdType.MESH,
        ).start()


def arrive(kind, target, sizes, sent, landed):
    sx, sy, _ = sizes
    lead = (slice(None),) * (target.ndim - 5)
    extent = ((sx, sy, 2), (sx, 2, sizes[2] + 2), (2, sy, sizes[2] + 2), (2, 2, sizes[2] + 2))[kind]
    whole = target.at[lead + tuple(pl.ds(0, size) for size in extent)]
    pltpu.make_async_copy(whole, whole, sent.at[kind]).wait()
    pltpu.make_async_copy(whole, whole, landed.at[kind]).wait()


def halves(value):
    high = value.astype(jnp.bfloat16)
    return high, (value - high.astype(jnp.float32)).astype(jnp.bfloat16)


def kernel(
    mesh_counts,
    counts,
    positions,
    energy_ref,
    force_ref,
    held,
    raw,
    source,
    ext,
    gain_own,
    gain_ext,
    order,
    pieces_of,
    picks,
    far,
    weights,
    lanes_of,
    dense,
    piles,
    table_rows,
    table,
    fetch_sem,
    table_sem,
    sent,
    landed,
    gain_landed,
):
    sizes = gain_own.shape[:3]
    sx, sy, sz = sizes
    wide = gain_ext.shape[:3]
    wx, wy, wz = wide
    slots = source.shape[-1]
    cells = sx * sy * sz
    group_count = groups_of(slots)
    depth = picks.shape[1]
    each = -(-SLOTS // weights.shape[2])

    def held_at(c, g, i):
        return c, g, i // each, i % each

    fetches = [
        pltpu.make_async_copy(counts, held, fetch_sem.at[0]),
        pltpu.make_async_copy(positions, raw, fetch_sem.at[1]),
    ]
    for fetch in fetches:
        fetch.start()
    greet(mesh_counts)

    lane = lax.broadcasted_iota(jnp.int32, (cells, slots), 1)
    cell = lax.broadcasted_iota(jnp.int32, (cells, slots), 0)
    column_of = sum(((cell >= k * sz).astype(jnp.int32) for k in range(1, sx * sy)), jnp.zeros_like(cell))
    plane_of = sum(((column_of >= k * sy).astype(jnp.int32) for k in range(1, sx)), jnp.zeros_like(cell))
    spots = (plane_of, column_of - plane_of * sy, cell - column_of * sz)

    for fetch in fetches:
        fetch.wait()
    occupancy = jnp.zeros((cells, slots), jnp.int32)
    for x in range(sx):
        for y in range(sy):
            for z in range(sz):
                occupancy = jnp.where(cell == (x * sy + y) * sz + z, held[x, y, z], occupancy)
    filled = lane < occupancy
    seated = [
        jnp.where(filled, raw[k].reshape(cells, slots), SENTINEL) for k in range(3)
    ]
    for k in range(3):
        source[k] = seated[k].reshape(sizes + (1, slots))


    own = [
        jnp.where(
            filled,
            seated[k] + ((spots[k] + 1).astype(jnp.float32) - 0.5 * wide[k]),
            0.0,
        )
        for k in range(3)
    ]
    inner = tuple(slice(1, 1 + size) for size in sizes)
    for k in range(3):
        ext[(k,) + inner] = seated[k].reshape(sizes + (1, slots))

    upper = [(seated[k] >= 0.5).astype(jnp.int32) for k in range(3)]
    octant = jnp.where(filled, 4 * upper[0] + 2 * upper[1] + upper[2], OCTANTS)
    members = jnp.concatenate(
        [jnp.where(octant == o, 1.0, 0.0) for o in range(OCTANTS)], axis=0
    ).astype(jnp.bfloat16)
    before = lax.broadcasted_iota(jnp.int32, (slots, 2 * slots), 0)
    after = lax.broadcasted_iota(jnp.int32, (slots, 2 * slots), 1)
    earlier = jnp.where((after >= slots) | (before < after), 1.0, 0.0).astype(jnp.bfloat16)
    ranks = jnp.dot(members, earlier, preferred_element_type=jnp.float32).astype(jnp.int32)
    start = jnp.zeros((cells, slots), jnp.int32)
    place = jnp.full((cells, slots), -1, jnp.int32)
    block = jnp.zeros((cells, slots), jnp.int32)
    phase_of = lane // SPAN
    group = lane - phase_of * SPAN
    for o in range(OCTANTS):
        rows = ranks[o * cells : (o + 1) * cells]
        place = jnp.where(octant == o, start + rows[:, :slots], place)
        if o:
            block = block + jnp.where(group * ROWS >= start, 1, 0)
        start = start + ((rows[:, slots:] + (ROWS - 1)) & -ROWS)
    order[...] = place
    bits = [(block >> 2) & 1, (block >> 1) & 1, block & 1]
    far_x = jnp.where(phase_of >= 2, spots[0] + 2 * bits[0], spots[0] + 1)
    far_y = jnp.where((phase_of & 1) == 1, spots[1] + 2 * bits[1], spots[1] + 1)
    table_rows[...] = (far_x * wy + far_y) * wz + spots[2] + bits[2]
    tabulate = pltpu.make_async_copy(table_rows, table, table_sem)
    tabulate.start()

    near = 1.0 - 4.0 * (own[0] * own[0] + own[1] * own[1] + own[2] * own[2])
    for k, value in enumerate([8.0 * own[0], 8.0 * own[1], 8.0 * own[2], near]):
        for part, piece in enumerate(split(value)):
            pieces_of[part, k] = piece

    batch = next(n for n in (8, 4, 2, 1) if cells % n == 0)
    kind_row = lax.broadcasted_iota(jnp.int32, (16, 4 * slots), 0)
    kind_lane = lax.broadcasted_iota(jnp.int32, (16, 4 * slots), 1)
    smear = jnp.where(
        (kind_row < 12) & ((kind_row & 3) == kind_lane // slots), 1.0, 0.0
    ).astype(jnp.bfloat16)

    def sort_cells(i, carry):
        found = []
        for j in range(batch):
            c = i * batch + j
            spot = order[pl.ds(c, 1), :]
            target = lax.broadcasted_iota(jnp.int32, (depth, slots), 0)
            pick = jnp.where(target == spot, 1.0, 0.0).astype(jnp.bfloat16)
            picks[c] = pick
            rows = [pieces_of[part, k, pl.ds(c, 1), :] for part in range(3) for k in range(4)]
            rows += [jnp.zeros((4, slots), jnp.float32)]
            found.append(
                lax.dot_general(
                    pick,
                    jnp.concatenate(rows, axis=0).astype(jnp.bfloat16),
                    (((1,), (1,)), ((), ())),
                    preferred_element_type=jnp.float32,
                ).astype(jnp.bfloat16)
            )
        for j in range(batch):
            spread = jnp.dot(found[j], smear, preferred_element_type=jnp.float32)
            for k in range(4):
                for g in range(group_count):
                    lanes_of[held_at(i * batch + j, g, k)] = spread[
                        g * ROWS : (g + 1) * ROWS, k * slots : (k + 1) * slots
                    ]
        return carry

    lax.fori_loop(0, cells // batch, sort_cells, 0)
    meet(mesh_counts)
    send_rims(mesh_counts, source, ext, sent, landed)

    def prepare(x, y, z, count):
        shape = (count, 1, slots)
        rows = [ext[k, x, y, pl.ds(z, count)] for k in range(3)]
        there = rows[0] < 2.0
        floor = lax.broadcasted_iota(jnp.int32, shape, 0).astype(jnp.float32) + (z - 0.5 * wz)
        shifts = (
            lax.convert_element_type(x, jnp.float32) - 0.5 * wx,
            lax.convert_element_type(y, jnp.float32) - 0.5 * wy,
            floor,
        )
        coords = [jnp.where(there, row + shift, 0.0) for row, shift in zip(rows, shifts)]
        squares = coords[0] * coords[0] + coords[1] * coords[1] + coords[2] * coords[2]
        at = pl.ds((x * wy + y) * wz + z, count)
        for k in range(3):
            far[at, 3, k : k + 1] = coords[k]
        far[at, 3, 3:4] = jnp.where(there, -4.0 * squares, FAR)

    def prepare_gain(x, y, z, count):
        far[pl.ds((x * wy + y) * wz + z, count), 3, 4:5] = gain_ext[x, y, pl.ds(z, count)]

    def far_row(at, k):
        return jnp.broadcast_to(far[at, 3, k : k + 1], (ROWS, slots))

    def columns(count, where, body):
        def step(i, carry):
            body(*where(i))
            return carry

        lax.fori_loop(0, count, step, 0)

    def inner_columns(body):
        columns(sx * sy, lambda i: (i // sy + 1, i % sy + 1), lambda x, y: body(x, y, 1, sz))

    def end_columns(body):
        def ends(x, y):
            body(x, y, 0, 1)
            body(x, y, wz - 1, 1)

        columns(sx * sy, lambda i: (i // sy + 1, i % sy + 1), ends)

    def plane_columns(body):
        columns(
            2 * sx, lambda i: (i // 2 + 1, i % 2 * (wy - 1)), lambda x, y: body(x, y, 0, wz)
        )

    def side_columns(ys, count, body):
        columns(
            2 * count,
            lambda i: (i // count * (wx - 1), ys(i % count)),
            lambda x, y: body(x, y, 0, wz),
        )

    def face_columns(body):
        side_columns(lambda y: y + 1, sy, body)

    def edge_columns(body):
        side_columns(lambda y: y * (wy - 1), 2, body)

    slot_lane = lax.broadcasted_iota(jnp.int32, (ROWS, slots), 1)

    def lane_sums(c, rows, parts):
        kept = dense[rows, :]
        for k, part in enumerate(parts):
            kept = jnp.where(
                slot_lane == k * cells + c, jnp.sum(part, axis=1, keepdims=True), kept
            )
        dense[rows, :] = kept

    def sorted_rows(kinds):
        flat = dense[...].T
        return [flat[k * cells : (k + 1) * cells, :depth] for k in range(kinds)]

    def batched(count, most, where, body, phases):
        several = next(n for n in range(most, 0, -1) if count % n == 0)

        def step(i, carry):
            for j in range(several):
                body(where(i * several + j), phases)
            return carry

        lax.fori_loop(0, count // several, step, 0)

    def all_cells(body, *phases):
        batched(cells, 4, lambda i: i, body, phases)

    def last_cells(body, *phases):
        batched(cells, 8, lambda i: i, body, phases)

    def middle_cells(body):
        span = sz - 2
        if span > 0:
            batched(sx * sy * span, 2, lambda i: i // span * sz + 1 + i % span, body, (0,))

    def end_cells(body):
        ends = min(sz, 2)
        columns(
            ends * sx * sy,
            lambda i: (i // ends * sz + i % ends * (sz - 1),),
            lambda c: body(c, (0,)),
        )

    def density(c, phases):
        def one_group(g, inside):
            xi, yi, zi, ci = (lanes_of[held_at(c, g, k)] for k in range(4))
            if phases[0]:
                rho, quartic = lanes_of[held_at(c, g, 4)], lanes_of[held_at(c, g, 5)]
            else:
                rho, quartic = (jnp.zeros((ROWS, slots), jnp.float32),) * 2
            for phase in phases:
                base = table[c, phase * SPAN + g]
                for step in range(2):
                    at = base + step
                    t = (far_row(at, 3) + ci) + xi * far_row(at, 0)
                    t = t + yi * far_row(at, 1) + zi * far_row(at, 2)
                    w = jnp.maximum(t, 0.0)
                    weights[held_at(c, g, 2 * phase + step)] = w
                    s = w * w
                    rho = rho + s
                    quartic = quartic + s * s
            if phases[-1] == 3:
                lane_sums(c, pl.ds(g * ROWS, ROWS), (rho, quartic))
            else:
                lanes_of[held_at(c, g, 4)] = rho
                lanes_of[held_at(c, g, 5)] = quartic
            return inside

        lax.fori_loop(0, group_count, one_group, 0, unroll=True)

    def force(c, phases):
        def one_group(g, inside):
            gi = lanes_of[held_at(c, g, 3)]
            if phases[0]:
                parts = [lanes_of[held_at(c, g, 4 + k)] for k in range(4)]
            else:
                parts = [jnp.zeros((ROWS, slots), jnp.float32)] * 4
            for phase in phases:
                base = table[c, phase * SPAN + g]
                for step in range(2):
                    at = base + step
                    w = weights[held_at(c, g, 2 * phase + step)]
                    f = w * ((far_row(at, 4) + gi) - w * w)
                    for k in range(3):
                        parts[k] = parts[k] + f * far_row(at, k)
                    parts[3] = parts[3] + f
            if phases[-1] == 3:
                whole = 0.125 * parts[3]
                parts = [parts[k] - lanes_of[held_at(c, g, k)] * whole for k in range(3)]
                lane_sums(c, pl.ds(g * ROWS, ROWS), parts)
            else:
                for k in range(4):
                    lanes_of[held_at(c, g, 4 + k)] = parts[k]
            return inside

        lax.fori_loop(0, group_count, one_group, 0, unroll=True)

    def unsort(kinds):
        pieces = [piece for value in kinds for piece in halves(value)]
        pieces = jnp.concatenate(pieces, axis=0)
        tall = pieces.shape[0]
        row = lax.broadcasted_iota(jnp.int32, pieces.shape, 0) % cells
        for lot in range(lots):
            total = jnp.zeros((tall, pair * slots), jnp.float32)
            for c in range(lot * cells // lots, (lot + 1) * cells // lots, pair):
                kept = jnp.where((row >= c) & (row < c + pair), pieces, jnp.zeros_like(pieces))
                both = jnp.concatenate([picks[c + j] for j in range(pair)], axis=1)
                total = total + jnp.dot(kept, both, preferred_element_type=jnp.float32)
            piles[lot, :tall] = total
        total = sum(piles[lot, :tall] for lot in range(lots))
        odd = lax.broadcasted_iota(jnp.int32, (tall, slots), 0) % pair
        total = functools.reduce(
            lambda kept, j: jnp.where(odd == j, total[:, j * slots : (j + 1) * slots], kept),
            range(1, pair),
            total[:, :slots],
        )
        rows = [total[k * cells : (k + 1) * cells] for k in range(2 * len(kinds))]
        return [rows[2 * k] + rows[2 * k + 1] for k in range(len(kinds))]

    pair = 2 if cells % 2 == 0 else 1
    lots = 2 if cells % 4 == 0 else 1

    def land(kind):
        arrive(kind, ext, sizes, sent, landed)

    def land_gain(kind):
        arrive(kind, gain_ext, sizes, sent, gain_landed)

    dense[...] = jnp.zeros_like(dense)
    inner_columns(prepare)
    tabulate.wait()
    middle_cells(density)
    land(0)
    end_columns(prepare)
    end_cells(density)
    land(1)
    plane_columns(prepare)
    all_cells(density, 1)
    land(2)
    face_columns(prepare)
    all_cells(density, 2)
    land(3)
    edge_columns(prepare)
    last_cells(density, 3)

    rho_rows, quartic_rows = sorted_rows(2)
    first = jnp.maximum(rho_rows - 1.0, 0.0)
    second = jnp.maximum(quartic_rows - 1.0, 0.0)
    fprime = -0.5 * EMBED_SCALE * lax.rsqrt(first + 1.0)
    gain = 0.5 - fprime * (0.5 / PAIR_SCALE)
    gain_rows = unsort([gain])[0]
    gain_own[...] = gain_rows.reshape(sizes + (1, slots))
    send_rims(mesh_counts, gain_own, gain_ext, sent, gain_landed)
    gain_ext[inner] = gain_rows.reshape(sizes + (1, slots))
    pair_sum = PAIR_SCALE * (second - 2.0 * first)
    energy = -EMBED_SCALE * jnp.sqrt(first + 1.0) + 0.5 * pair_sum
    energy_rows = unsort([energy])[0]
    energy_ref[...] = jnp.where(filled, energy_rows, 0.0).reshape(sizes + (slots,))

    tall = [piece.astype(jnp.float32) for piece in halves(gain)]
    tall += [jnp.zeros((slots - 2 * cells, depth), jnp.float32)]
    tall = jnp.concatenate(tall, axis=0)
    tall = jnp.concatenate([tall, jnp.zeros((slots, -depth % 128), jnp.float32)], axis=1)
    standing = tall.T[:depth].astype(jnp.bfloat16)
    pick_row = lax.broadcasted_iota(jnp.int32, (slots, pair * slots), 0)
    pick_cell = jnp.where(
        pick_row < 2 * cells, pick_row - jnp.where(pick_row >= cells, cells, 0), -1
    )
    pick_lane = lax.broadcasted_iota(jnp.int32, (slots, pair * slots), 1) // slots
    for i in range(cells // pair):
        chosen = jnp.where(pick_cell == pair * i + pick_lane, 1.0, 0.0).astype(jnp.bfloat16)
        spread = jnp.dot(standing, chosen, preferred_element_type=jnp.float32)
        for j in range(pair):
            for g in range(group_count):
                lanes_of[held_at(pair * i + j, g, 3)] = spread[
                    g * ROWS : (g + 1) * ROWS, j * slots : (j + 1) * slots
                ]

    inner_columns(prepare_gain)
    middle_cells(force)
    land_gain(0)
    end_columns(prepare_gain)
    end_cells(force)
    land_gain(1)
    plane_columns(prepare_gain)
    all_cells(force, 1)
    land_gain(2)
    face_columns(prepare_gain)
    land_gain(3)
    edge_columns(prepare_gain)
    last_cells(force, 2, 3)

    scale = FORCE_SCALE * 4.0 * PAIR_SCALE
    pushes = unsort(sorted_rows(3))
    for k, push in enumerate(pushes):
        force_ref[k] = jnp.where(filled, scale * push, 0.0).reshape(sizes + (slots,))


def groups_of(slots):
    return (slots + OCTANTS * (ROWS - 1)) // ROWS


def hand_over(energy, force, energy_out, force_out, done):
    copies = [
        pltpu.make_async_copy(force, force_out, done.at[0]),
        pltpu.make_async_copy(energy, energy_out, done.at[1]),
    ]
    for copy in copies:
        copy.start()
    for copy in copies:
        copy.wait()


def per_device(mesh_counts, positions, counts):
    slots = positions.shape[-1]
    sizes = positions.shape[1:4]
    wide = tuple(size + 2 for size in sizes)
    cells = sizes[0] * sizes[1] * sizes[2]
    far_cells = wide[0] * wide[1] * wide[2]
    groups = groups_of(slots)
    depth = -(-groups // 2) * 2 * ROWS
    f32, bf16, i32 = jnp.float32, jnp.bfloat16, jnp.int32
    roomy = 2 * cells * groups * -(-SLOTS // 3) * 16 * ROWS * slots <= 40 << 20
    quads = -(-SLOTS // (3 if roomy else 4))
    vmem = [
        ((3,) + sizes + (slots,), f32),
        ((3,) + sizes + (1, slots), f32),
        ((3,) + wide + (1, slots), f32),
        (sizes + (1, slots), f32),
        (wide + (1, slots), f32),
        ((cells, slots), i32),
        ((3, 4, cells, slots), f32),
        ((cells, depth, slots), bf16),
        ((far_cells, 4, ROWS, slots), f32),
        ((cells, groups, quads, 4, ROWS, slots), f32),
        ((cells, groups, quads, 4, ROWS, slots), f32),
        ((-(-depth // 128) * 128, slots), f32),
        ((2, 6 * cells, 2 * slots), f32),
        ((cells, slots), i32),
    ]
    held = sum(math.prod(shape) * jnp.dtype(kind).itemsize for shape, kind in vmem)
    results = pl.pallas_call(
        functools.partial(kernel, mesh_counts),
        out_shape=(
            jax.ShapeDtypeStruct(sizes + (slots,), f32),
            jax.ShapeDtypeStruct((3,) + sizes + (slots,), f32),
        ),
        in_specs=[pl.BlockSpec(memory_space=pltpu.HBM)] * 2,
        out_specs=(pl.BlockSpec(memory_space=pltpu.VMEM),) * 2,
        scratch_shapes=[pltpu.SMEM(counts.shape, i32)]
        + [pltpu.VMEM(shape, kind) for shape, kind in vmem]
        + [
            pltpu.SMEM((cells, slots), i32),
            pltpu.SemaphoreType.DMA((2,)),
            pltpu.SemaphoreType.DMA,
        ]
        + [pltpu.SemaphoreType.DMA((4,))] * 3,
        compiler_params=pltpu.CompilerParams(
            collective_id=0,
            has_side_effects=True,
            vmem_limit_bytes=held + (4 << 20),
        ),
        name="atoms",
    )(*(pltpu.with_memory_space_constraint(x, pltpu.HBM) for x in (counts, positions)))
    return pl.pallas_call(
        hand_over,
        out_shape=tuple(jax.ShapeDtypeStruct(x.shape, x.dtype) for x in results),
        in_specs=[pl.BlockSpec(memory_space=pltpu.VMEM)] * 2,
        out_specs=(pl.BlockSpec(memory_space=pl.ANY),) * 2,
        scratch_shapes=[pltpu.SemaphoreType.DMA((2,))],
        compiler_params=pltpu.CompilerParams(vmem_limit_bytes=1 << 20),
        name="hand",
    )(*results)


def solution(mesh):
    placed = (P(None, "gx", "gy", "gz", None), P("gx", "gy", "gz"))
    return jax.shard_map(
        functools.partial(per_device, tuple(mesh.shape[name] for name in NAMES)),
        mesh=mesh,
        in_specs=placed,
        out_specs=(P("gx", "gy", "gz", None), P(None, "gx", "gy", "gz", None)),
        check_vma=False,
    )
```

```python
import functools
import math

import jax
import jax.numpy as jnp
from jax import lax
from jax.experimental import pallas as pl
from jax.experimental.pallas import tpu as pltpu
from jax.sharding import PartitionSpec as P

SENTINEL = 4.0
PAIR_SCALE = 0.02
EMBED_SCALE = 0.2
FORCE_SCALE = 8.0
FAR = -1.0e6
ROWS = 8
OCTANTS = 8
SPAN = 32
SLOTS = 8


def split(value):
    first = value.astype(jnp.bfloat16).astype(jnp.float32)
    rest = value - first
    second = rest.astype(jnp.bfloat16).astype(jnp.float32)
    return first, second, rest - second


NAMES = ("gx", "gy", "gz")
DIRECTIONS = [
    (x, y, z) for x in (-1, 0, 1) for y in (-1, 0, 1) for z in (-1, 0, 1) if (x, y, z) != (0, 0, 0)
]
DIRECTIONS.sort(key=lambda step: (abs(step[0]) * (1 + abs(step[1])), -sum(map(abs, step))))


def device_at(counts, step):
    return {
        name: lax.rem(lax.axis_index(name) + (offset + count), count)
        for name, offset, count in zip(NAMES, step, counts)
    }


def partners(counts):
    return sorted(
        {tuple(o % c for o, c in zip(step, counts)) for step in DIRECTIONS},
        key=lambda step: [-min(o, c - o) for o, c in zip(step, counts)],
    )


def greet(counts):
    barrier = pltpu.get_barrier_semaphore()
    for step in partners(counts):
        pl.semaphore_signal(
            barrier,
            inc=1,
            device_id=device_at(counts, step),
            device_id_type=pl.DeviceIdType.MESH,
        )


def meet(counts):
    pl.semaphore_wait(pltpu.get_barrier_semaphore(), len(partners(counts)))


def kind_of(step):
    return (2 if step[0] else 0) + (1 if step[1] else 0)


def send_rims(counts, source, target, sent, landed):
    lead = (slice(None),) * (source.ndim - 5)
    sizes = source.shape[-5:-2]
    for step in DIRECTIONS:
        here = tuple(
            pl.ds(0, size) if o == 0 else pl.ds(size - 1 if o > 0 else 0, 1)
            for o, size in zip(step, sizes)
        )
        there = tuple(
            pl.ds(1, size) if o == 0 else pl.ds(0 if o > 0 else size + 1, 1)
            for o, size in zip(step, sizes)
        )
        pltpu.make_async_remote_copy(
            src_ref=source.at[lead + here],
            dst_ref=target.at[lead + there],
            send_sem=sent.at[kind_of(step)],
            recv_sem=landed.at[kind_of(step)],
            device_id=device_at(counts, step),
            device_id_type=pl.DeviceIdType.MESH,
        ).start()


def arrive(kind, target, sizes, sent, landed):
    sx, sy, _ = sizes
    lead = (slice(None),) * (target.ndim - 5)
    extent = ((sx, sy, 2), (sx, 2, sizes[2] + 2), (2, sy, sizes[2] + 2), (2, 2, sizes[2] + 2))[kind]
    whole = target.at[lead + tuple(pl.ds(0, size) for size in extent)]
    pltpu.make_async_copy(whole, whole, sent.at[kind]).wait()
    pltpu.make_async_copy(whole, whole, landed.at[kind]).wait()


def halves(value):
    high = value.astype(jnp.bfloat16)
    return high, (value - high.astype(jnp.float32)).astype(jnp.bfloat16)


def kernel(
    mesh_counts,
    counts,
    positions,
    energy_ref,
    force_ref,
    held,
    raw,
    source,
    ext,
    gain_own,
    gain_ext,
    order,
    pieces_of,
    picks,
    far,
    weights,
    lanes_of,
    dense,
    piles,
    table_rows,
    table,
    fetch_sem,
    table_sem,
    sent,
    landed,
    gain_landed,
):
    sizes = gain_own.shape[:3]
    sx, sy, sz = sizes
    wide = gain_ext.shape[:3]
    wx, wy, wz = wide
    slots = source.shape[-1]
    cells = sx * sy * sz
    group_count = groups_of(slots)
    depth = picks.shape[1]
    each = -(-SLOTS // weights.shape[2])

    def held_at(c, g, i):
        return c, g, i // each, i % each

    fetches = [
        pltpu.make_async_copy(counts, held, fetch_sem.at[0]),
        pltpu.make_async_copy(positions, raw, fetch_sem.at[1]),
    ]
    for fetch in fetches:
        fetch.start()
    greet(mesh_counts)

    lane = lax.broadcasted_iota(jnp.int32, (cells, slots), 1)
    cell = lax.broadcasted_iota(jnp.int32, (cells, slots), 0)
    column_of = sum(((cell >= k * sz).astype(jnp.int32) for k in range(1, sx * sy)), jnp.zeros_like(cell))
    plane_of = sum(((column_of >= k * sy).astype(jnp.int32) for k in range(1, sx)), jnp.zeros_like(cell))
    spots = (plane_of, column_of - plane_of * sy, cell - column_of * sz)

    for fetch in fetches:
        fetch.wait()
    occupancy = jnp.zeros((cells, slots), jnp.int32)
    for x in range(sx):
        for y in range(sy):
            for z in range(sz):
                occupancy = jnp.where(cell == (x * sy + y) * sz + z, held[x, y, z], occupancy)
    filled = lane < occupancy
    seated = [
        jnp.where(filled, raw[k].reshape(cells, slots), SENTINEL) for k in range(3)
    ]
    for k in range(3):
        source[k] = seated[k].reshape(sizes + (1, slots))


    own = [
        jnp.where(
            filled,
            seated[k] + ((spots[k] + 1).astype(jnp.float32) - 0.5 * wide[k]),
            0.0,
        )
        for k in range(3)
    ]
    inner = tuple(slice(1, 1 + size) for size in sizes)
    for k in range(3):
        ext[(k,) + inner] = seated[k].reshape(sizes + (1, slots))

    upper = [(seated[k] >= 0.5).astype(jnp.int32) for k in range(3)]
    octant = jnp.where(filled, 4 * upper[0] + 2 * upper[1] + upper[2], OCTANTS)
    members = jnp.concatenate(
        [jnp.where(octant == o, 1.0, 0.0) for o in range(OCTANTS)], axis=0
    ).astype(jnp.bfloat16)
    before = lax.broadcasted_iota(jnp.int32, (slots, 2 * slots), 0)
    after = lax.broadcasted_iota(jnp.int32, (slots, 2 * slots), 1)
    earlier = jnp.where((after >= slots) | (before < after), 1.0, 0.0).astype(jnp.bfloat16)
    ranks = jnp.dot(members, earlier, preferred_element_type=jnp.float32).astype(jnp.int32)
    start = jnp.zeros((cells, slots), jnp.int32)
    place = jnp.full((cells, slots), -1, jnp.int32)
    block = jnp.zeros((cells, slots), jnp.int32)
    phase_of = lane // SPAN
    group = lane - phase_of * SPAN
    for o in range(OCTANTS):
        rows = ranks[o * cells : (o + 1) * cells]
        place = jnp.where(octant == o, start + rows[:, :slots], place)
        if o:
            block = block + jnp.where(group * ROWS >= start, 1, 0)
        start = start + ((rows[:, slots:] + (ROWS - 1)) & -ROWS)
    order[...] = place
    bits = [(block >> 2) & 1, (block >> 1) & 1, block & 1]
    far_x = jnp.where(phase_of >= 2, spots[0] + 2 * bits[0], spots[0] + 1)
    far_y = jnp.where((phase_of & 1) == 1, spots[1] + 2 * bits[1], spots[1] + 1)
    table_rows[...] = (far_x * wy + far_y) * wz + spots[2] + bits[2]
    tabulate = pltpu.make_async_copy(table_rows, table, table_sem)
    tabulate.start()

    near = 1.0 - 4.0 * (own[0] * own[0] + own[1] * own[1] + own[2] * own[2])
    for k, value in enumerate([8.0 * own[0], 8.0 * own[1], 8.0 * own[2], near]):
        for part, piece in enumerate(split(value)):
            pieces_of[part, k] = piece

    batch = next(n for n in (8, 4, 2, 1) if cells % n == 0)
    kind_row = lax.broadcasted_iota(jnp.int32, (16, 4 * slots), 0)
    kind_lane = lax.broadcasted_iota(jnp.int32, (16, 4 * slots), 1)
    smear = jnp.where(
        (kind_row < 12) & ((kind_row & 3) == kind_lane // slots), 1.0, 0.0
    ).astype(jnp.bfloat16)

    def sort_cells(i, carry):
        found = []
        for j in range(batch):
            c = i * batch + j
            spot = order[pl.ds(c, 1), :]
            target = lax.broadcasted_iota(jnp.int32, (depth, slots), 0)
            pick = jnp.where(target == spot, 1.0, 0.0).astype(jnp.bfloat16)
            picks[c] = pick
            rows = [pieces_of[part, k, pl.ds(c, 1), :] for part in range(3) for k in range(4)]
            rows += [jnp.zeros((4, slots), jnp.float32)]
            found.append(
                lax.dot_general(
                    pick,
                    jnp.concatenate(rows, axis=0).astype(jnp.bfloat16),
                    (((1,), (1,)), ((), ())),
                    preferred_element_type=jnp.float32,
                ).astype(jnp.bfloat16)
            )
        for j in range(batch):
            spread = jnp.dot(found[j], smear, preferred_element_type=jnp.float32)
            for k in range(4):
                for g in range(group_count):
                    lanes_of[held_at(i * batch + j, g, k)] = spread[
                        g * ROWS : (g + 1) * ROWS, k * slots : (k + 1) * slots
                    ]
        return carry

    lax.fori_loop(0, cells // batch, sort_cells, 0)
    meet(mesh_counts)
    send_rims(mesh_counts, source, ext, sent, landed)

    def prepare(x, y, z, count):
        shape = (count, 1, slots)
        rows = [ext[k, x, y, pl.ds(z, count)] for k in range(3)]
        there = rows[0] < 2.0
        floor = lax.broadcasted_iota(jnp.int32, shape, 0).astype(jnp.float32) + (z - 0.5 * wz)
        shifts = (
            lax.convert_element_type(x, jnp.float32) - 0.5 * wx,
            lax.convert_element_type(y, jnp.float32) - 0.5 * wy,
            floor,
        )
        coords = [jnp.where(there, row + shift, 0.0) for row, shift in zip(rows, shifts)]
        squares = coords[0] * coords[0] + coords[1] * coords[1] + coords[2] * coords[2]
        at = pl.ds((x * wy + y) * wz + z, count)
        for k in range(3):
            far[at, 3, k : k + 1] = coords[k]
        far[at, 3, 3:4] = jnp.where(there, -4.0 * squares, FAR)

    def prepare_gain(x, y, z, count):
        far[pl.ds((x * wy + y) * wz + z, count), 3, 4:5] = gain_ext[x, y, pl.ds(z, count)]

    def far_row(at, k):
        return jnp.broadcast_to(far[at, 3, k : k + 1], (ROWS, slots))

    def columns(count, where, body):
        several = next(n for n in (4, 2, 1) if count % n == 0)

        def step(i, carry):
            for j in range(several):
                body(*where(i * several + j))
            return carry

        lax.fori_loop(0, count // several, step, 0)

    def inner_columns(body):
        columns(sx * sy, lambda i: (i // sy + 1, i % sy + 1), lambda x, y: body(x, y, 1, sz))

    def end_columns(body):
        def ends(x, y):
            body(x, y, 0, 1)
            body(x, y, wz - 1, 1)

        columns(sx * sy, lambda i: (i // sy + 1, i % sy + 1), ends)

    def plane_columns(body):
        columns(
            2 * sx, lambda i: (i // 2 + 1, i % 2 * (wy - 1)), lambda x, y: body(x, y, 0, wz)
        )

    def side_columns(ys, count, body):
        columns(
            2 * count,
            lambda i: (i // count * (wx - 1), ys(i % count)),
            lambda x, y: body(x, y, 0, wz),
        )

    def face_columns(body):
        side_columns(lambda y: y + 1, sy, body)

    def edge_columns(body):
        side_columns(lambda y: y * (wy - 1), 2, body)

    slot_lane = lax.broadcasted_iota(jnp.int32, (ROWS, slots), 1)

    def lane_sums(c, rows, parts):
        kept = dense[rows, :]
        for k, part in enumerate(parts):
            kept = jnp.where(
                slot_lane == k * cells + c, jnp.sum(part, axis=1, keepdims=True), kept
            )
        dense[rows, :] = kept

    def sorted_rows(kinds):
        flat = dense[...].T
        return [flat[k * cells : (k + 1) * cells, :depth] for k in range(kinds)]

    def batched(count, most, where, body, phases):
        several = next(n for n in range(most, 0, -1) if count % n == 0)

        def step(i, carry):
            for j in range(several):
                body(where(i * several + j), phases)
            return carry

        lax.fori_loop(0, count // several, step, 0)

    def all_cells(body, *phases):
        batched(cells, 4, lambda i: i, body, phases)

    def last_cells(body, *phases):
        batched(cells, 8, lambda i: i, body, phases)

    def middle_cells(body):
        span = sz - 2
        if span > 0:
            batched(sx * sy * span, 4, lambda i: i // span * sz + 1 + i % span, body, (0,))

    def end_cells(body):
        ends = min(sz, 2)
        batched(ends * sx * sy, 4, lambda i: i // ends * sz + i % ends * (sz - 1), body, (0,))

    def density(c, phases):
        def one_group(g, inside):
            xi, yi, zi, ci = (lanes_of[held_at(c, g, k)] for k in range(4))
            if phases[0]:
                rho, quartic = lanes_of[held_at(c, g, 4)], lanes_of[held_at(c, g, 5)]
            else:
                rho, quartic = (jnp.zeros((ROWS, slots), jnp.float32),) * 2
            for phase in phases:
                base = table[c, phase * SPAN + g]
                for step in range(2):
                    at = base + step
                    t = (far_row(at, 3) + ci) + xi * far_row(at, 0)
                    t = t + yi * far_row(at, 1) + zi * far_row(at, 2)
                    w = jnp.maximum(t, 0.0)
                    weights[held_at(c, g, 2 * phase + step)] = w
                    s = w * w
                    rho = rho + s
                    quartic = quartic + s * s
            if phases[-1] == 3:
                lane_sums(c, pl.ds(g * ROWS, ROWS), (rho, quartic))
            else:
                lanes_of[held_at(c, g, 4)] = rho
                lanes_of[held_at(c, g, 5)] = quartic
            return inside

        lax.fori_loop(0, group_count, one_group, 0, unroll=True)

    def force(c, phases):
        def one_group(g, inside):
            gi = lanes_of[held_at(c, g, 3)]
            if phases[0]:
                parts = [lanes_of[held_at(c, g, 4 + k)] for k in range(4)]
            else:
                parts = [jnp.zeros((ROWS, slots), jnp.float32)] * 4
            for phase in phases:
                base = table[c, phase * SPAN + g]
                for step in range(2):
                    at = base + step
                    w = weights[held_at(c, g, 2 * phase + step)]
                    f = w * ((far_row(at, 4) + gi) - w * w)
                    for k in range(3):
                        parts[k] = parts[k] + f * far_row(at, k)
                    parts[3] = parts[3] + f
            if phases[-1] == 3:
                whole = 0.125 * parts[3]
                parts = [parts[k] - lanes_of[held_at(c, g, k)] * whole for k in range(3)]
                lane_sums(c, pl.ds(g * ROWS, ROWS), parts)
            else:
                for k in range(4):
                    lanes_of[held_at(c, g, 4 + k)] = parts[k]
            return inside

        lax.fori_loop(0, group_count, one_group, 0, unroll=True)

    def unsort(kinds):
        pieces = [piece for value in kinds for piece in halves(value)]
        pieces = jnp.concatenate(pieces, axis=0)
        tall = pieces.shape[0]
        row = lax.broadcasted_iota(jnp.int32, pieces.shape, 0) % cells
        for lot in range(lots):
            total = jnp.zeros((tall, pair * slots), jnp.float32)
            for c in range(lot * cells // lots, (lot + 1) * cells // lots, pair):
                kept = jnp.where((row >= c) & (row < c + pair), pieces, jnp.zeros_like(pieces))
                both = jnp.concatenate([picks[c + j] for j in range(pair)], axis=1)
                total = total + jnp.dot(kept, both, preferred_element_type=jnp.float32)
            piles[lot, :tall] = total
        total = sum(piles[lot, :tall] for lot in range(lots))
        odd = lax.broadcasted_iota(jnp.int32, (tall, slots), 0) % pair
        total = functools.reduce(
            lambda kept, j: jnp.where(odd == j, total[:, j * slots : (j + 1) * slots], kept),
            range(1, pair),
            total[:, :slots],
        )
        rows = [total[k * cells : (k + 1) * cells] for k in range(2 * len(kinds))]
        return [rows[2 * k] + rows[2 * k + 1] for k in range(len(kinds))]

    pair = 2 if cells % 2 == 0 else 1
    lots = 2 if cells % 4 == 0 else 1

    def land(kind):
        arrive(kind, ext, sizes, sent, landed)

    def land_gain(kind):
        arrive(kind, gain_ext, sizes, sent, gain_landed)

    dense[...] = jnp.zeros_like(dense)
    inner_columns(prepare)
    tabulate.wait()
    middle_cells(density)
    land(0)
    end_columns(prepare)
    end_cells(density)
    land(1)
    plane_columns(prepare)
    all_cells(density, 1)
    land(2)
    face_columns(prepare)
    all_cells(density, 2)
    land(3)
    edge_columns(prepare)
    last_cells(density, 3)

    rho_rows, quartic_rows = sorted_rows(2)
    first = jnp.maximum(rho_rows - 1.0, 0.0)
    second = jnp.maximum(quartic_rows - 1.0, 0.0)
    fprime = -0.5 * EMBED_SCALE * lax.rsqrt(first + 1.0)
    gain = 0.5 - fprime * (0.5 / PAIR_SCALE)
    gain_rows = unsort([gain])[0]
    gain_own[...] = gain_rows.reshape(sizes + (1, slots))
    send_rims(mesh_counts, gain_own, gain_ext, sent, gain_landed)
    gain_ext[inner] = gain_rows.reshape(sizes + (1, slots))
    pair_sum = PAIR_SCALE * (second - 2.0 * first)
    energy = -EMBED_SCALE * jnp.sqrt(first + 1.0) + 0.5 * pair_sum
    energy_rows = unsort([energy])[0]
    energy_ref[...] = jnp.where(filled, energy_rows, 0.0).reshape(sizes + (slots,))

    tall = [piece.astype(jnp.float32) for piece in halves(gain)]
    tall += [jnp.zeros((slots - 2 * cells, depth), jnp.float32)]
    tall = jnp.concatenate(tall, axis=0)
    tall = jnp.concatenate([tall, jnp.zeros((slots, -depth % 128), jnp.float32)], axis=1)
    standing = tall.T[:depth].astype(jnp.bfloat16)
    pick_row = lax.broadcasted_iota(jnp.int32, (slots, pair * slots), 0)
    pick_cell = jnp.where(
        pick_row < 2 * cells, pick_row - jnp.where(pick_row >= cells, cells, 0), -1
    )
    pick_lane = lax.broadcasted_iota(jnp.int32, (slots, pair * slots), 1) // slots
    for i in range(cells // pair):
        chosen = jnp.where(pick_cell == pair * i + pick_lane, 1.0, 0.0).astype(jnp.bfloat16)
        spread = jnp.dot(standing, chosen, preferred_element_type=jnp.float32)
        for j in range(pair):
            for g in range(group_count):
                lanes_of[held_at(pair * i + j, g, 3)] = spread[
                    g * ROWS : (g + 1) * ROWS, j * slots : (j + 1) * slots
                ]

    inner_columns(prepare_gain)
    middle_cells(force)
    land_gain(0)
    end_columns(prepare_gain)
    end_cells(force)
    land_gain(1)
    plane_columns(prepare_gain)
    all_cells(force, 1)
    land_gain(2)
    face_columns(prepare_gain)
    all_cells(force, 2)
    land_gain(3)
    edge_columns(prepare_gain)
    last_cells(force, 3)

    scale = FORCE_SCALE * 4.0 * PAIR_SCALE
    pushes = unsort(sorted_rows(3))
    for k, push in enumerate(pushes):
        force_ref[k] = jnp.where(filled, scale * push, 0.0).reshape(sizes + (slots,))


def groups_of(slots):
    return (slots + OCTANTS * (ROWS - 1)) // ROWS


def hand_over(energy, force, energy_out, force_out, done):
    copies = [
        pltpu.make_async_copy(force, force_out, done.at[0]),
        pltpu.make_async_copy(energy, energy_out, done.at[1]),
    ]
    for copy in copies:
        copy.start()
    for copy in copies:
        copy.wait()


def per_device(mesh_counts, positions, counts):
    slots = positions.shape[-1]
    sizes = positions.shape[1:4]
    wide = tuple(size + 2 for size in sizes)
    cells = sizes[0] * sizes[1] * sizes[2]
    far_cells = wide[0] * wide[1] * wide[2]
    groups = groups_of(slots)
    depth = -(-groups // 2) * 2 * ROWS
    f32, bf16, i32 = jnp.float32, jnp.bfloat16, jnp.int32
    roomy = 2 * cells * groups * -(-SLOTS // 3) * 16 * ROWS * slots <= 40 << 20
    quads = -(-SLOTS // (3 if roomy else 4))
    vmem = [
        ((3,) + sizes + (slots,), f32),
        ((3,) + sizes + (1, slots), f32),
        ((3,) + wide + (1, slots), f32),
        (sizes + (1, slots), f32),
        (wide + (1, slots), f32),
        ((cells, slots), i32),
        ((3, 4, cells, slots), f32),
        ((cells, depth, slots), bf16),
        ((far_cells, 4, ROWS, slots), f32),
        ((cells, groups, quads, 4, ROWS, slots), f32),
        ((cells, groups, quads, 4, ROWS, slots), f32),
        ((-(-depth // 128) * 128, slots), f32),
        ((2, 6 * cells, 2 * slots), f32),
        ((cells, slots), i32),
    ]
    held = sum(math.prod(shape) * jnp.dtype(kind).itemsize for shape, kind in vmem)
    results = pl.pallas_call(
        functools.partial(kernel, mesh_counts),
        out_shape=(
            jax.ShapeDtypeStruct(sizes + (slots,), f32),
            jax.ShapeDtypeStruct((3,) + sizes + (slots,), f32),
        ),
        in_specs=[pl.BlockSpec(memory_space=pltpu.HBM)] * 2,
        out_specs=(pl.BlockSpec(memory_space=pltpu.VMEM),) * 2,
        scratch_shapes=[pltpu.SMEM(counts.shape, i32)]
        + [pltpu.VMEM(shape, kind) for shape, kind in vmem]
        + [
            pltpu.SMEM((cells, slots), i32),
            pltpu.SemaphoreType.DMA((2,)),
            pltpu.SemaphoreType.DMA,
        ]
        + [pltpu.SemaphoreType.DMA((4,))] * 3,
        compiler_params=pltpu.CompilerParams(
            collective_id=0,
            has_side_effects=True,
            vmem_limit_bytes=held + (4 << 20),
        ),
        name="atoms",
    )(*(pltpu.with_memory_space_constraint(x, pltpu.HBM) for x in (counts, positions)))
    return pl.pallas_call(
        hand_over,
        out_shape=tuple(jax.ShapeDtypeStruct(x.shape, x.dtype) for x in results),
        in_specs=[pl.BlockSpec(memory_space=pltpu.VMEM)] * 2,
        out_specs=(pl.BlockSpec(memory_space=pl.ANY),) * 2,
        scratch_shapes=[pltpu.SemaphoreType.DMA((2,))],
        compiler_params=pltpu.CompilerParams(vmem_limit_bytes=1 << 20),
        name="hand",
    )(*results)


def solution(mesh):
    placed = (P(None, "gx", "gy", "gz", None), P("gx", "gy", "gz"))
    return jax.shard_map(
        functools.partial(per_device, tuple(mesh.shape[name] for name in NAMES)),
        mesh=mesh,
        in_specs=placed,
        out_specs=(P("gx", "gy", "gz", None), P(None, "gx", "gy", "gz", None)),
        check_vma=False,
    )
```

```python
import functools
import math

import jax
import jax.numpy as jnp
from jax import lax
from jax.experimental import pallas as pl
from jax.experimental.pallas import tpu as pltpu
from jax.sharding import PartitionSpec as P

SENTINEL = 4.0
PAIR_SCALE = 0.02
EMBED_SCALE = 0.2
FORCE_SCALE = 8.0
FAR = -1.0e6
ROWS = 8
OCTANTS = 8
SPAN = 32
SLOTS = 8


def split(value):
    first = value.astype(jnp.bfloat16).astype(jnp.float32)
    rest = value - first
    second = rest.astype(jnp.bfloat16).astype(jnp.float32)
    return first, second, rest - second


NAMES = ("gx", "gy", "gz")
DIRECTIONS = [
    (x, y, z) for x in (-1, 0, 1) for y in (-1, 0, 1) for z in (-1, 0, 1) if (x, y, z) != (0, 0, 0)
]
DIRECTIONS.sort(key=lambda step: (abs(step[0]) * (1 + abs(step[1])), -sum(map(abs, step))))


def device_at(counts, step):
    return {
        name: lax.rem(lax.axis_index(name) + (offset + count), count)
        for name, offset, count in zip(NAMES, step, counts)
    }


def partners(counts):
    return sorted(
        {tuple(o % c for o, c in zip(step, counts)) for step in DIRECTIONS},
        key=lambda step: [-min(o, c - o) for o, c in zip(step, counts)],
    )


def greet(counts):
    barrier = pltpu.get_barrier_semaphore()
    for step in partners(counts):
        pl.semaphore_signal(
            barrier,
            inc=1,
            device_id=device_at(counts, step),
            device_id_type=pl.DeviceIdType.MESH,
        )


def meet(counts):
    pl.semaphore_wait(pltpu.get_barrier_semaphore(), len(partners(counts)))


def kind_of(step):
    return (2 if step[0] else 0) + (1 if step[1] else 0)


def send_rims(counts, source, target, sent, landed):
    lead = (slice(None),) * (source.ndim - 5)
    sizes = source.shape[-5:-2]
    for step in DIRECTIONS:
        here = tuple(
            pl.ds(0, size) if o == 0 else pl.ds(size - 1 if o > 0 else 0, 1)
            for o, size in zip(step, sizes)
        )
        there = tuple(
            pl.ds(1, size) if o == 0 else pl.ds(0 if o > 0 else size + 1, 1)
            for o, size in zip(step, sizes)
        )
        pltpu.make_async_remote_copy(
            src_ref=source.at[lead + here],
            dst_ref=target.at[lead + there],
            send_sem=sent.at[kind_of(step)],
            recv_sem=landed.at[kind_of(step)],
            device_id=device_at(counts, step),
            device_id_type=pl.DeviceIdType.MESH,
        ).start()


def arrive(kind, target, sizes, sent, landed):
    sx, sy, _ = sizes
    lead = (slice(None),) * (target.ndim - 5)
    extent = ((sx, sy, 2), (sx, 2, sizes[2] + 2), (2, sy, sizes[2] + 2), (2, 2, sizes[2] + 2))[kind]
    whole = target.at[lead + tuple(pl.ds(0, size) for size in extent)]
    pltpu.make_async_copy(whole, whole, sent.at[kind]).wait()
    pltpu.make_async_copy(whole, whole, landed.at[kind]).wait()


def halves(value):
    high = value.astype(jnp.bfloat16)
    return high, (value - high.astype(jnp.float32)).astype(jnp.bfloat16)


def kernel(
    mesh_counts,
    counts,
    positions,
    energy_ref,
    force_ref,
    held,
    raw,
    source,
    ext,
    gain_own,
    gain_ext,
    order,
    pieces_of,
    picks,
    far,
    weights,
    lanes_of,
    dense,
    piles,
    table_rows,
    table,
    fetch_sem,
    table_sem,
    sent,
    landed,
    gain_landed,
):
    sizes = gain_own.shape[:3]
    sx, sy, sz = sizes
    wide = gain_ext.shape[:3]
    wx, wy, wz = wide
    slots = source.shape[-1]
    cells = sx * sy * sz
    group_count = groups_of(slots)
    depth = picks.shape[1]
    each = -(-SLOTS // weights.shape[2])

    def held_at(c, g, i):
        return c, g, i // each, i % each

    fetches = [
        pltpu.make_async_copy(counts, held, fetch_sem.at[0]),
        pltpu.make_async_copy(positions, raw, fetch_sem.at[1]),
    ]
    for fetch in fetches:
        fetch.start()
    greet(mesh_counts)

    lane = lax.broadcasted_iota(jnp.int32, (cells, slots), 1)
    cell = lax.broadcasted_iota(jnp.int32, (cells, slots), 0)
    column_of = sum(((cell >= k * sz).astype(jnp.int32) for k in range(1, sx * sy)), jnp.zeros_like(cell))
    plane_of = sum(((column_of >= k * sy).astype(jnp.int32) for k in range(1, sx)), jnp.zeros_like(cell))
    spots = (plane_of, column_of - plane_of * sy, cell - column_of * sz)

    for fetch in fetches:
        fetch.wait()
    occupancy = jnp.zeros((cells, slots), jnp.int32)
    for x in range(sx):
        for y in range(sy):
            for z in range(sz):
                occupancy = jnp.where(cell == (x * sy + y) * sz + z, held[x, y, z], occupancy)
    filled = lane < occupancy
    seated = [
        jnp.where(filled, raw[k].reshape(cells, slots), SENTINEL) for k in range(3)
    ]
    for k in range(3):
        source[k] = seated[k].reshape(sizes + (1, slots))


    own = [
        jnp.where(
            filled,
            seated[k] + ((spots[k] + 1).astype(jnp.float32) - 0.5 * wide[k]),
            0.0,
        )
        for k in range(3)
    ]
    inner = tuple(slice(1, 1 + size) for size in sizes)
    for k in range(3):
        ext[(k,) + inner] = seated[k].reshape(sizes + (1, slots))

    upper = [(seated[k] >= 0.5).astype(jnp.int32) for k in range(3)]
    octant = jnp.where(filled, 4 * upper[0] + 2 * upper[1] + upper[2], OCTANTS)
    members = jnp.concatenate(
        [jnp.where(octant == o, 1.0, 0.0) for o in range(OCTANTS)], axis=0
    ).astype(jnp.bfloat16)
    before = lax.broadcasted_iota(jnp.int32, (slots, 2 * slots), 0)
    after = lax.broadcasted_iota(jnp.int32, (slots, 2 * slots), 1)
    earlier = jnp.where((after >= slots) | (before < after), 1.0, 0.0).astype(jnp.bfloat16)
    ranks = jnp.dot(members, earlier, preferred_element_type=jnp.float32).astype(jnp.int32)
    start = jnp.zeros((cells, slots), jnp.int32)
    place = jnp.full((cells, slots), -1, jnp.int32)
    block = jnp.zeros((cells, slots), jnp.int32)
    phase_of = lane // SPAN
    group = lane - phase_of * SPAN
    for o in range(OCTANTS):
        rows = ranks[o * cells : (o + 1) * cells]
        place = jnp.where(octant == o, start + rows[:, :slots], place)
        if o:
            block = block + jnp.where(group * ROWS >= start, 1, 0)
        start = start + ((rows[:, slots:] + (ROWS - 1)) & -ROWS)
    order[...] = place
    bits = [(block >> 2) & 1, (block >> 1) & 1, block & 1]
    far_x = jnp.where(phase_of >= 2, spots[0] + 2 * bits[0], spots[0] + 1)
    far_y = jnp.where((phase_of & 1) == 1, spots[1] + 2 * bits[1], spots[1] + 1)
    table_rows[...] = (far_x * wy + far_y) * wz + spots[2] + bits[2]
    tabulate = pltpu.make_async_copy(table_rows, table, table_sem)
    tabulate.start()

    near = 1.0 - 4.0 * (own[0] * own[0] + own[1] * own[1] + own[2] * own[2])
    for k, value in enumerate([8.0 * own[0], 8.0 * own[1], 8.0 * own[2], near]):
        for part, piece in enumerate(split(value)):
            pieces_of[part, k] = piece

    batch = next(n for n in (8, 4, 2, 1) if cells % n == 0)
    kind_row = lax.broadcasted_iota(jnp.int32, (16, 4 * slots), 0)
    kind_lane = lax.broadcasted_iota(jnp.int32, (16, 4 * slots), 1)
    smear = jnp.where(
        (kind_row < 12) & ((kind_row & 3) == kind_lane // slots), 1.0, 0.0
    ).astype(jnp.bfloat16)

    def sort_cells(i, carry):
        found = []
        for j in range(batch):
            c = i * batch + j
            spot = order[pl.ds(c, 1), :]
            target = lax.broadcasted_iota(jnp.int32, (depth, slots), 0)
            pick = jnp.where(target == spot, 1.0, 0.0).astype(jnp.bfloat16)
            picks[c] = pick
            rows = [pieces_of[part, k, pl.ds(c, 1), :] for part in range(3) for k in range(4)]
            rows += [jnp.zeros((4, slots), jnp.float32)]
            found.append(
                lax.dot_general(
                    pick,
                    jnp.concatenate(rows, axis=0).astype(jnp.bfloat16),
                    (((1,), (1,)), ((), ())),
                    preferred_element_type=jnp.float32,
                ).astype(jnp.bfloat16)
            )
        for j in range(batch):
            spread = jnp.dot(found[j], smear, preferred_element_type=jnp.float32)
            for k in range(4):
                for g in range(group_count):
                    lanes_of[held_at(i * batch + j, g, k)] = spread[
                        g * ROWS : (g + 1) * ROWS, k * slots : (k + 1) * slots
                    ]
        return carry

    lax.fori_loop(0, cells // batch, sort_cells, 0)
    meet(mesh_counts)
    send_rims(mesh_counts, source, ext, sent, landed)

    def prepare(x, y, z, count):
        shape = (count, 1, slots)
        rows = [ext[k, x, y, pl.ds(z, count)] for k in range(3)]
        there = rows[0] < 2.0
        floor = lax.broadcasted_iota(jnp.int32, shape, 0).astype(jnp.float32) + (z - 0.5 * wz)
        shifts = (
            lax.convert_element_type(x, jnp.float32) - 0.5 * wx,
            lax.convert_element_type(y, jnp.float32) - 0.5 * wy,
            floor,
        )
        coords = [jnp.where(there, row + shift, 0.0) for row, shift in zip(rows, shifts)]
        squares = coords[0] * coords[0] + coords[1] * coords[1] + coords[2] * coords[2]
        at = pl.ds((x * wy + y) * wz + z, count)
        for k in range(3):
            far[at, 3, k : k + 1] = coords[k]
        far[at, 3, 3:4] = jnp.where(there, -4.0 * squares, FAR)

    def prepare_gain(x, y, z, count):
        far[pl.ds((x * wy + y) * wz + z, count), 3, 4:5] = gain_ext[x, y, pl.ds(z, count)]

    def far_row(at, k):
        return jnp.broadcast_to(far[at, 3, k : k + 1], (ROWS, slots))

    def columns(count, where, body):
        several = next(n for n in (4, 2, 1) if count % n == 0)

        def step(i, carry):
            for j in range(several):
                body(*where(i * several + j))
            return carry

        lax.fori_loop(0, count // several, step, 0)

    def inner_columns(body):
        columns(sx * sy, lambda i: (i // sy + 1, i % sy + 1), lambda x, y: body(x, y, 1, sz))

    def end_columns(body):
        def ends(x, y):
            body(x, y, 0, 1)
            body(x, y, wz - 1, 1)

        columns(sx * sy, lambda i: (i // sy + 1, i % sy + 1), ends)

    def plane_columns(body):
        columns(
            2 * sx, lambda i: (i // 2 + 1, i % 2 * (wy - 1)), lambda x, y: body(x, y, 0, wz)
        )

    def side_columns(ys, count, body):
        columns(
            2 * count,
            lambda i: (i // count * (wx - 1), ys(i % count)),
            lambda x, y: body(x, y, 0, wz),
        )

    def face_columns(body):
        side_columns(lambda y: y + 1, sy, body)

    def edge_columns(body):
        side_columns(lambda y: y * (wy - 1), 2, body)

    slot_lane = lax.broadcasted_iota(jnp.int32, (ROWS, slots), 1)

    def lane_sums(c, rows, parts, kind=0):
        kept = dense[rows, :]
        for k, part in enumerate(parts, kind):
            kept = jnp.where(
                slot_lane == k * cells + c, jnp.sum(part, axis=1, keepdims=True), kept
            )
        dense[rows, :] = kept

    def sorted_rows(kinds):
        flat = dense[...].T
        return [flat[k * cells : (k + 1) * cells, :depth] for k in range(kinds)]

    def batched(count, most, where, body, phases):
        several = next(n for n in range(most, 0, -1) if count % n == 0)

        def step(i, carry):
            for j in range(several):
                body(where(i * several + j), phases)
            return carry

        lax.fori_loop(0, count // several, step, 0)

    def all_cells(body, *phases):
        batched(cells, 4, lambda i: i, body, phases)

    def last_cells(body, *phases):
        batched(cells, 8, lambda i: i, body, phases)

    def middle_cells(body):
        span = sz - 2
        if span > 0:
            batched(sx * sy * span, 4, lambda i: i // span * sz + 1 + i % span, body, (0,))

    def end_cells(body):
        ends = min(sz, 2)
        batched(ends * sx * sy, 4, lambda i: i // ends * sz + i % ends * (sz - 1), body, (0,))

    def density(c, phases):
        def one_group(g, inside):
            xi, yi, zi, ci = (lanes_of[held_at(c, g, k)] for k in range(4))
            early = phases[0] == 0
            if early:
                rho, quartic = (jnp.zeros((ROWS, slots), jnp.float32),) * 2
            else:
                rho = lanes_of[held_at(c, g, 4)]
            for phase in phases:
                base = table[c, phase * SPAN + g]
                for step in range(2):
                    at = base + step
                    t = (far_row(at, 3) + ci) + xi * far_row(at, 0)
                    t = t + yi * far_row(at, 1) + zi * far_row(at, 2)
                    w = jnp.maximum(t, 0.0)
                    weights[held_at(c, g, 2 * phase + step)] = w
                    s = w * w
                    rho = rho + s
                    if early:
                        quartic = quartic + s * s
            if phases[-1] == 3:
                lane_sums(c, pl.ds(g * ROWS, ROWS), (rho,))
            else:
                lanes_of[held_at(c, g, 4)] = rho
            if early:
                lanes_of[held_at(c, g, 5)] = quartic
            return inside

        lax.fori_loop(0, group_count, one_group, 0, unroll=True)

    def quartics(c, phases):
        def one_group(g, inside):
            quartic = lanes_of[held_at(c, g, 5)]
            for i in range(2, 8):
                w = weights[held_at(c, g, i)]
                s = w * w
                quartic = quartic + s * s
            lane_sums(c, pl.ds(g * ROWS, ROWS), (quartic,), 1)
            return inside

        lax.fori_loop(0, group_count, one_group, 0, unroll=True)

    def force(c, phases):
        def one_group(g, inside):
            gi = lanes_of[held_at(c, g, 3)]
            if phases[0]:
                parts = [lanes_of[held_at(c, g, 4 + k)] for k in range(4)]
            else:
                parts = [jnp.zeros((ROWS, slots), jnp.float32)] * 4
            for phase in phases:
                base = table[c, phase * SPAN + g]
                for step in range(2):
                    at = base + step
                    w = weights[held_at(c, g, 2 * phase + step)]
                    f = w * ((far_row(at, 4) + gi) - w * w)
                    for k in range(3):
                        parts[k] = parts[k] + f * far_row(at, k)
                    parts[3] = parts[3] + f
            if phases[-1] == 3:
                whole = 0.125 * parts[3]
                parts = [parts[k] - lanes_of[held_at(c, g, k)] * whole for k in range(3)]
                lane_sums(c, pl.ds(g * ROWS, ROWS), parts)
            else:
                for k in range(4):
                    lanes_of[held_at(c, g, 4 + k)] = parts[k]
            return inside

        lax.fori_loop(0, group_count, one_group, 0, unroll=True)

    def unsort(kinds):
        pieces = [piece for value in kinds for piece in halves(value)]
        pieces = jnp.concatenate(pieces, axis=0)
        tall = pieces.shape[0]
        row = lax.broadcasted_iota(jnp.int32, pieces.shape, 0) % cells
        for lot in range(lots):
            total = jnp.zeros((tall, pair * slots), jnp.float32)
            for c in range(lot * cells // lots, (lot + 1) * cells // lots, pair):
                kept = jnp.where((row >= c) & (row < c + pair), pieces, jnp.zeros_like(pieces))
                both = jnp.concatenate([picks[c + j] for j in range(pair)], axis=1)
                total = total + jnp.dot(kept, both, preferred_element_type=jnp.float32)
            piles[lot, :tall] = total
        total = sum(piles[lot, :tall] for lot in range(lots))
        odd = lax.broadcasted_iota(jnp.int32, (tall, slots), 0) % pair
        total = functools.reduce(
            lambda kept, j: jnp.where(odd == j, total[:, j * slots : (j + 1) * slots], kept),
            range(1, pair),
            total[:, :slots],
        )
        rows = [total[k * cells : (k + 1) * cells] for k in range(2 * len(kinds))]
        return [rows[2 * k] + rows[2 * k + 1] for k in range(len(kinds))]

    pair = 2 if cells % 2 == 0 else 1
    lots = 2 if cells % 4 == 0 else 1

    def land(kind):
        arrive(kind, ext, sizes, sent, landed)

    def land_gain(kind):
        arrive(kind, gain_ext, sizes, sent, gain_landed)

    dense[...] = jnp.zeros_like(dense)
    inner_columns(prepare)
    tabulate.wait()
    middle_cells(density)
    land(0)
    end_columns(prepare)
    end_cells(density)
    land(1)
    plane_columns(prepare)
    all_cells(density, 1)
    land(2)
    face_columns(prepare)
    all_cells(density, 2)
    land(3)
    edge_columns(prepare)
    last_cells(density, 3)

    rho_rows = sorted_rows(1)[0]
    first = jnp.maximum(rho_rows - 1.0, 0.0)
    fprime = -0.5 * EMBED_SCALE * lax.rsqrt(first + 1.0)
    gain = 0.5 - fprime * (0.5 / PAIR_SCALE)
    gain_rows = unsort([gain])[0]
    gain_own[...] = gain_rows.reshape(sizes + (1, slots))
    send_rims(mesh_counts, gain_own, gain_ext, sent, gain_landed)
    gain_ext[inner] = gain_rows.reshape(sizes + (1, slots))
    tall = [piece.astype(jnp.float32) for piece in halves(gain)]
    tall += [jnp.zeros((slots - 2 * cells, depth), jnp.float32)]
    tall = jnp.concatenate(tall, axis=0)
    tall = jnp.concatenate([tall, jnp.zeros((slots, -depth % 128), jnp.float32)], axis=1)
    standing = tall.T[:depth].astype(jnp.bfloat16)
    pick_row = lax.broadcasted_iota(jnp.int32, (slots, pair * slots), 0)
    pick_cell = jnp.where(
        pick_row < 2 * cells, pick_row - jnp.where(pick_row >= cells, cells, 0), -1
    )
    pick_lane = lax.broadcasted_iota(jnp.int32, (slots, pair * slots), 1) // slots
    for i in range(cells // pair):
        chosen = jnp.where(pick_cell == pair * i + pick_lane, 1.0, 0.0).astype(jnp.bfloat16)
        spread = jnp.dot(standing, chosen, preferred_element_type=jnp.float32)
        for j in range(pair):
            for g in range(group_count):
                lanes_of[held_at(pair * i + j, g, 3)] = spread[
                    g * ROWS : (g + 1) * ROWS, j * slots : (j + 1) * slots
                ]

    last_cells(quartics)
    second = jnp.maximum(sorted_rows(2)[1] - 1.0, 0.0)
    pair_sum = PAIR_SCALE * (second - 2.0 * first)
    energy = -EMBED_SCALE * jnp.sqrt(first + 1.0) + 0.5 * pair_sum
    energy_rows = unsort([energy])[0]
    energy_ref[...] = jnp.where(filled, energy_rows, 0.0).reshape(sizes + (slots,))

    inner_columns(prepare_gain)
    middle_cells(force)
    land_gain(0)
    end_columns(prepare_gain)
    end_cells(force)
    land_gain(1)
    plane_columns(prepare_gain)
    all_cells(force, 1)
    land_gain(2)
    face_columns(prepare_gain)
    all_cells(force, 2)
    land_gain(3)
    edge_columns(prepare_gain)
    last_cells(force, 3)

    scale = FORCE_SCALE * 4.0 * PAIR_SCALE
    pushes = unsort(sorted_rows(3))
    for k, push in enumerate(pushes):
        force_ref[k] = jnp.where(filled, scale * push, 0.0).reshape(sizes + (slots,))


def groups_of(slots):
    return (slots + OCTANTS * (ROWS - 1)) // ROWS


def hand_over(energy, force, energy_out, force_out, done):
    copies = [
        pltpu.make_async_copy(force, force_out, done.at[0]),
        pltpu.make_async_copy(energy, energy_out, done.at[1]),
    ]
    for copy in copies:
        copy.start()
    for copy in copies:
        copy.wait()


def per_device(mesh_counts, positions, counts):
    slots = positions.shape[-1]
    sizes = positions.shape[1:4]
    wide = tuple(size + 2 for size in sizes)
    cells = sizes[0] * sizes[1] * sizes[2]
    far_cells = wide[0] * wide[1] * wide[2]
    groups = groups_of(slots)
    depth = -(-groups // 2) * 2 * ROWS
    f32, bf16, i32 = jnp.float32, jnp.bfloat16, jnp.int32
    roomy = 2 * cells * groups * -(-SLOTS // 3) * 16 * ROWS * slots <= 40 << 20
    quads = -(-SLOTS // (3 if roomy else 4))
    vmem = [
        ((3,) + sizes + (slots,), f32),
        ((3,) + sizes + (1, slots), f32),
        ((3,) + wide + (1, slots), f32),
        (sizes + (1, slots), f32),
        (wide + (1, slots), f32),
        ((cells, slots), i32),
        ((3, 4, cells, slots), f32),
        ((cells, depth, slots), bf16),
        ((far_cells, 4, ROWS, slots), f32),
        ((cells, groups, quads, 4, ROWS, slots), f32),
        ((cells, groups, quads, 4, ROWS, slots), f32),
        ((-(-depth // 128) * 128, slots), f32),
        ((2, 6 * cells, 2 * slots), f32),
        ((cells, slots), i32),
    ]
    held = sum(math.prod(shape) * jnp.dtype(kind).itemsize for shape, kind in vmem)
    results = pl.pallas_call(
        functools.partial(kernel, mesh_counts),
        out_shape=(
            jax.ShapeDtypeStruct(sizes + (slots,), f32),
            jax.ShapeDtypeStruct((3,) + sizes + (slots,), f32),
        ),
        in_specs=[pl.BlockSpec(memory_space=pltpu.HBM)] * 2,
        out_specs=(pl.BlockSpec(memory_space=pltpu.VMEM),) * 2,
        scratch_shapes=[pltpu.SMEM(counts.shape, i32)]
        + [pltpu.VMEM(shape, kind) for shape, kind in vmem]
        + [
            pltpu.SMEM((cells, slots), i32),
            pltpu.SemaphoreType.DMA((2,)),
            pltpu.SemaphoreType.DMA,
        ]
        + [pltpu.SemaphoreType.DMA((4,))] * 3,
        compiler_params=pltpu.CompilerParams(
            collective_id=0,
            has_side_effects=True,
            vmem_limit_bytes=held + (4 << 20),
        ),
        name="atoms",
    )(*(pltpu.with_memory_space_constraint(x, pltpu.HBM) for x in (counts, positions)))
    return pl.pallas_call(
        hand_over,
        out_shape=tuple(jax.ShapeDtypeStruct(x.shape, x.dtype) for x in results),
        in_specs=[pl.BlockSpec(memory_space=pltpu.VMEM)] * 2,
        out_specs=(pl.BlockSpec(memory_space=pl.ANY),) * 2,
        scratch_shapes=[pltpu.SemaphoreType.DMA((2,))],
        compiler_params=pltpu.CompilerParams(vmem_limit_bytes=1 << 20),
        name="hand",
    )(*results)


def solution(mesh):
    placed = (P(None, "gx", "gy", "gz", None), P("gx", "gy", "gz"))
    return jax.shard_map(
        functools.partial(per_device, tuple(mesh.shape[name] for name in NAMES)),
        mesh=mesh,
        in_specs=placed,
        out_specs=(P("gx", "gy", "gz", None), P(None, "gx", "gy", "gz", None)),
        check_vma=False,
    )
```

```python
import functools
import math

import jax
import jax.numpy as jnp
from jax import lax
from jax.experimental import pallas as pl
from jax.experimental.pallas import tpu as pltpu
from jax.sharding import PartitionSpec as P

SENTINEL = 4.0
PAIR_SCALE = 0.02
EMBED_SCALE = 0.2
FORCE_SCALE = 8.0
FAR = -1.0e6
ROWS = 8
OCTANTS = 8
SPAN = 32
SLOTS = 8


def split(value):
    first = value.astype(jnp.bfloat16).astype(jnp.float32)
    rest = value - first
    second = rest.astype(jnp.bfloat16).astype(jnp.float32)
    return first, second, rest - second


NAMES = ("gx", "gy", "gz")
DIRECTIONS = [
    (x, y, z) for x in (-1, 0, 1) for y in (-1, 0, 1) for z in (-1, 0, 1) if (x, y, z) != (0, 0, 0)
]
DIRECTIONS.sort(key=lambda step: (abs(step[0]) * (1 + abs(step[1])), -sum(map(abs, step))))


def device_at(counts, step):
    return {
        name: lax.rem(lax.axis_index(name) + (offset + count), count)
        for name, offset, count in zip(NAMES, step, counts)
    }


def partners(counts):
    return sorted(
        {tuple(o % c for o, c in zip(step, counts)) for step in DIRECTIONS},
        key=lambda step: [-min(o, c - o) for o, c in zip(step, counts)],
    )


def greet(counts):
    barrier = pltpu.get_barrier_semaphore()
    for step in partners(counts):
        pl.semaphore_signal(
            barrier,
            inc=1,
            device_id=device_at(counts, step),
            device_id_type=pl.DeviceIdType.MESH,
        )


def meet(counts):
    pl.semaphore_wait(pltpu.get_barrier_semaphore(), len(partners(counts)))


def kind_of(step):
    return (2 if step[0] else 0) + (1 if step[1] else 0)


def send_rims(counts, source, target, sent, landed):
    lead = (slice(None),) * (source.ndim - 5)
    sizes = source.shape[-5:-2]
    for step in DIRECTIONS:
        here = tuple(
            pl.ds(0, size) if o == 0 else pl.ds(size - 1 if o > 0 else 0, 1)
            for o, size in zip(step, sizes)
        )
        there = tuple(
            pl.ds(1, size) if o == 0 else pl.ds(0 if o > 0 else size + 1, 1)
            for o, size in zip(step, sizes)
        )
        pltpu.make_async_remote_copy(
            src_ref=source.at[lead + here],
            dst_ref=target.at[lead + there],
            send_sem=sent.at[kind_of(step)],
            recv_sem=landed.at[kind_of(step)],
            device_id=device_at(counts, step),
            device_id_type=pl.DeviceIdType.MESH,
        ).start()


def arrive(kind, target, sizes, sent, landed):
    sx, sy, _ = sizes
    lead = (slice(None),) * (target.ndim - 5)
    extent = ((sx, sy, 2), (sx, 2, sizes[2] + 2), (2, sy, sizes[2] + 2), (2, 2, sizes[2] + 2))[kind]
    whole = target.at[lead + tuple(pl.ds(0, size) for size in extent)]
    pltpu.make_async_copy(whole, whole, sent.at[kind]).wait()
    pltpu.make_async_copy(whole, whole, landed.at[kind]).wait()


def halves(value):
    high = value.astype(jnp.bfloat16)
    return high, (value - high.astype(jnp.float32)).astype(jnp.bfloat16)


def kernel(
    mesh_counts,
    counts,
    positions,
    energy_ref,
    force_ref,
    held,
    raw,
    source,
    ext,
    gain_own,
    gain_ext,
    order,
    pieces_of,
    picks,
    far,
    weights,
    lanes_of,
    dense,
    piles,
    table_rows,
    table,
    fetch_sem,
    table_sem,
    sent,
    landed,
    gain_landed,
):
    sizes = gain_own.shape[:3]
    sx, sy, sz = sizes
    wide = gain_ext.shape[:3]
    wx, wy, wz = wide
    slots = source.shape[-1]
    cells = sx * sy * sz
    group_count = groups_of(slots)
    depth = picks.shape[1]
    each = -(-SLOTS // weights.shape[2])

    def held_at(c, g, i):
        return c, g, i // each, i % each

    fetches = [
        pltpu.make_async_copy(counts, held, fetch_sem.at[0]),
        pltpu.make_async_copy(positions, raw, fetch_sem.at[1]),
    ]
    for fetch in fetches:
        fetch.start()
    greet(mesh_counts)

    lane = lax.broadcasted_iota(jnp.int32, (cells, slots), 1)
    cell = lax.broadcasted_iota(jnp.int32, (cells, slots), 0)
    column_of = sum(((cell >= k * sz).astype(jnp.int32) for k in range(1, sx * sy)), jnp.zeros_like(cell))
    plane_of = sum(((column_of >= k * sy).astype(jnp.int32) for k in range(1, sx)), jnp.zeros_like(cell))
    spots = (plane_of, column_of - plane_of * sy, cell - column_of * sz)

    for fetch in fetches:
        fetch.wait()
    occupancy = jnp.zeros((cells, slots), jnp.int32)
    for x in range(sx):
        for y in range(sy):
            for z in range(sz):
                occupancy = jnp.where(cell == (x * sy + y) * sz + z, held[x, y, z], occupancy)
    filled = lane < occupancy
    seated = [
        jnp.where(filled, raw[k].reshape(cells, slots), SENTINEL) for k in range(3)
    ]
    for k in range(3):
        source[k] = seated[k].reshape(sizes + (1, slots))


    own = [
        jnp.where(
            filled,
            seated[k] + ((spots[k] + 1).astype(jnp.float32) - 0.5 * wide[k]),
            0.0,
        )
        for k in range(3)
    ]
    inner = tuple(slice(1, 1 + size) for size in sizes)
    for k in range(3):
        ext[(k,) + inner] = seated[k].reshape(sizes + (1, slots))

    upper = [(seated[k] >= 0.5).astype(jnp.int32) for k in range(3)]
    octant = jnp.where(filled, 4 * upper[0] + 2 * upper[1] + upper[2], OCTANTS)
    members = jnp.concatenate(
        [jnp.where(octant == o, 1.0, 0.0) for o in range(OCTANTS)], axis=0
    ).astype(jnp.bfloat16)
    before = lax.broadcasted_iota(jnp.int32, (slots, 2 * slots), 0)
    after = lax.broadcasted_iota(jnp.int32, (slots, 2 * slots), 1)
    earlier = jnp.where((after >= slots) | (before < after), 1.0, 0.0).astype(jnp.bfloat16)
    ranks = jnp.dot(members, earlier, preferred_element_type=jnp.float32).astype(jnp.int32)
    start = jnp.zeros((cells, slots), jnp.int32)
    place = jnp.full((cells, slots), -1, jnp.int32)
    block = jnp.zeros((cells, slots), jnp.int32)
    phase_of = lane // SPAN
    group = lane - phase_of * SPAN
    for o in range(OCTANTS):
        rows = ranks[o * cells : (o + 1) * cells]
        place = jnp.where(octant == o, start + rows[:, :slots], place)
        if o:
            block = block + jnp.where(group * ROWS >= start, 1, 0)
        start = start + ((rows[:, slots:] + (ROWS - 1)) & -ROWS)
    order[...] = place
    bits = [(block >> 2) & 1, (block >> 1) & 1, block & 1]
    far_x = jnp.where(phase_of >= 2, spots[0] + 2 * bits[0], spots[0] + 1)
    far_y = jnp.where((phase_of & 1) == 1, spots[1] + 2 * bits[1], spots[1] + 1)
    table_rows[...] = (far_x * wy + far_y) * wz + spots[2] + bits[2]
    tabulate = pltpu.make_async_copy(table_rows, table, table_sem)
    tabulate.start()

    near = 1.0 - 4.0 * (own[0] * own[0] + own[1] * own[1] + own[2] * own[2])
    for k, value in enumerate([8.0 * own[0], 8.0 * own[1], 8.0 * own[2], near]):
        for part, piece in enumerate(split(value)):
            pieces_of[part, k] = piece

    batch = next(n for n in (8, 4, 2, 1) if cells % n == 0)
    kind_row = lax.broadcasted_iota(jnp.int32, (16, 4 * slots), 0)
    kind_lane = lax.broadcasted_iota(jnp.int32, (16, 4 * slots), 1)
    smear = jnp.where(
        (kind_row < 12) & ((kind_row & 3) == kind_lane // slots), 1.0, 0.0
    ).astype(jnp.bfloat16)

    def sort_cells(i, carry):
        found = []
        for j in range(batch):
            c = i * batch + j
            spot = order[pl.ds(c, 1), :]
            target = lax.broadcasted_iota(jnp.int32, (depth, slots), 0)
            pick = jnp.where(target == spot, 1.0, 0.0).astype(jnp.bfloat16)
            picks[c] = pick
            rows = [pieces_of[part, k, pl.ds(c, 1), :] for part in range(3) for k in range(4)]
            rows += [jnp.zeros((4, slots), jnp.float32)]
            found.append(
                lax.dot_general(
                    pick,
                    jnp.concatenate(rows, axis=0).astype(jnp.bfloat16),
                    (((1,), (1,)), ((), ())),
                    preferred_element_type=jnp.float32,
                ).astype(jnp.bfloat16)
            )
        for j in range(batch):
            spread = jnp.dot(found[j], smear, preferred_element_type=jnp.float32)
            for k in range(4):
                for g in range(group_count):
                    lanes_of[held_at(i * batch + j, g, k)] = spread[
                        g * ROWS : (g + 1) * ROWS, k * slots : (k + 1) * slots
                    ]
        return carry

    lax.fori_loop(0, cells // batch, sort_cells, 0)
    meet(mesh_counts)
    send_rims(mesh_counts, source, ext, sent, landed)

    def prepare(x, y, z, count):
        shape = (count, 1, slots)
        rows = [ext[k, x, y, pl.ds(z, count)] for k in range(3)]
        there = rows[0] < 2.0
        floor = lax.broadcasted_iota(jnp.int32, shape, 0).astype(jnp.float32) + (z - 0.5 * wz)
        shifts = (
            lax.convert_element_type(x, jnp.float32) - 0.5 * wx,
            lax.convert_element_type(y, jnp.float32) - 0.5 * wy,
            floor,
        )
        coords = [jnp.where(there, row + shift, 0.0) for row, shift in zip(rows, shifts)]
        squares = coords[0] * coords[0] + coords[1] * coords[1] + coords[2] * coords[2]
        at = pl.ds((x * wy + y) * wz + z, count)
        for k in range(3):
            far[at, 3, k : k + 1] = coords[k]
        far[at, 3, 3:4] = jnp.where(there, -4.0 * squares, FAR)

    def prepare_gain(x, y, z, count):
        far[pl.ds((x * wy + y) * wz + z, count), 3, 4:5] = gain_ext[x, y, pl.ds(z, count)]

    def far_row(at, k):
        return jnp.broadcast_to(far[at, 3, k : k + 1], (ROWS, slots))

    def columns(count, where, body):
        several = next(n for n in (4, 2, 1) if count % n == 0)

        def step(i, carry):
            for j in range(several):
                body(*where(i * several + j))
            return carry

        lax.fori_loop(0, count // several, step, 0)

    def inner_columns(body):
        columns(sx * sy, lambda i: (i // sy + 1, i % sy + 1), lambda x, y: body(x, y, 1, sz))

    def end_columns(body):
        def ends(x, y):
            body(x, y, 0, 1)
            body(x, y, wz - 1, 1)

        columns(sx * sy, lambda i: (i // sy + 1, i % sy + 1), ends)

    def plane_columns(body):
        columns(
            2 * sx, lambda i: (i // 2 + 1, i % 2 * (wy - 1)), lambda x, y: body(x, y, 0, wz)
        )

    def side_columns(ys, count, body):
        columns(
            2 * count,
            lambda i: (i // count * (wx - 1), ys(i % count)),
            lambda x, y: body(x, y, 0, wz),
        )

    def face_columns(body):
        side_columns(lambda y: y + 1, sy, body)

    def edge_columns(body):
        side_columns(lambda y: y * (wy - 1), 2, body)

    slot_lane = lax.broadcasted_iota(jnp.int32, (ROWS, slots), 1)

    def lane_sums(c, rows, parts, kind=0):
        kept = dense[rows, :]
        for k, part in enumerate(parts, kind):
            kept = jnp.where(
                slot_lane == k * cells + c, jnp.sum(part, axis=1, keepdims=True), kept
            )
        dense[rows, :] = kept

    def sorted_rows(kinds):
        flat = dense[...].T
        return [flat[k * cells : (k + 1) * cells, :depth] for k in range(kinds)]

    def batched(count, most, where, body, phases):
        several = next(n for n in range(most, 0, -1) if count % n == 0)

        def step(i, carry):
            for j in range(several):
                body(where(i * several + j), phases)
            return carry

        lax.fori_loop(0, count // several, step, 0)

    def all_cells(body, *phases):
        batched(cells, 4, lambda i: i, body, phases)

    def last_cells(body, *phases):
        batched(cells, 8, lambda i: i, body, phases)

    def middle_cells(body):
        span = sz - 2
        if span > 0:
            batched(sx * sy * span, 4, lambda i: i // span * sz + 1 + i % span, body, (0,))

    def end_cells(body):
        ends = min(sz, 2)
        batched(ends * sx * sy, 4, lambda i: i // ends * sz + i % ends * (sz - 1), body, (0,))

    def density(c, phases):
        def one_group(g, inside):
            xi, yi, zi, ci = (lanes_of[held_at(c, g, k)] for k in range(4))
            early = phases[0] == 0
            if early:
                rho, quartic = (jnp.zeros((ROWS, slots), jnp.float32),) * 2
            else:
                rho = lanes_of[held_at(c, g, 4)]
            for phase in phases:
                base = table[c, phase * SPAN + g]
                for step in range(2):
                    at = base + step
                    t = (far_row(at, 3) + ci) + xi * far_row(at, 0)
                    t = t + yi * far_row(at, 1) + zi * far_row(at, 2)
                    w = jnp.maximum(t, 0.0)
                    weights[held_at(c, g, 2 * phase + step)] = w
                    s = w * w
                    rho = rho + s
                    if early:
                        quartic = quartic + s * s
            if phases[-1] == 3:
                lane_sums(c, pl.ds(g * ROWS, ROWS), (rho,))
            else:
                lanes_of[held_at(c, g, 4)] = rho
            if early:
                lanes_of[held_at(c, g, 5)] = quartic
            return inside

        lax.fori_loop(0, group_count, one_group, 0, unroll=True)

    def quartics(c, phases):
        def one_group(g, inside):
            quartic = lanes_of[held_at(c, g, 5)]
            for i in range(2, 8):
                w = weights[held_at(c, g, i)]
                s = w * w
                quartic = quartic + s * s
            lane_sums(c, pl.ds(g * ROWS, ROWS), (quartic,), 3)
            return inside

        lax.fori_loop(0, group_count, one_group, 0, unroll=True)

    def force(c, phases):
        def one_group(g, inside):
            gi = lanes_of[held_at(c, g, 3)]
            if phases[0]:
                parts = [lanes_of[held_at(c, g, 4 + k)] for k in range(4)]
            else:
                parts = [jnp.zeros((ROWS, slots), jnp.float32)] * 4
            for phase in phases:
                base = table[c, phase * SPAN + g]
                for step in range(2):
                    at = base + step
                    w = weights[held_at(c, g, 2 * phase + step)]
                    f = w * ((far_row(at, 4) + gi) - w * w)
                    for k in range(3):
                        parts[k] = parts[k] + f * far_row(at, k)
                    parts[3] = parts[3] + f
            if phases[-1] == 3:
                whole = 0.125 * parts[3]
                parts = [parts[k] - lanes_of[held_at(c, g, k)] * whole for k in range(3)]
                lane_sums(c, pl.ds(g * ROWS, ROWS), parts)
            else:
                for k in range(4):
                    lanes_of[held_at(c, g, 4 + k)] = parts[k]
            return inside

        lax.fori_loop(0, group_count, one_group, 0, unroll=True)

    def unsort(kinds):
        pieces = [piece for value in kinds for piece in halves(value)]
        pieces = jnp.concatenate(pieces, axis=0)
        tall = pieces.shape[0]
        row = lax.broadcasted_iota(jnp.int32, pieces.shape, 0) % cells
        for lot in range(lots):
            total = jnp.zeros((tall, pair * slots), jnp.float32)
            for c in range(lot * cells // lots, (lot + 1) * cells // lots, pair):
                kept = jnp.where((row >= c) & (row < c + pair), pieces, jnp.zeros_like(pieces))
                both = jnp.concatenate([picks[c + j] for j in range(pair)], axis=1)
                total = total + jnp.dot(kept, both, preferred_element_type=jnp.float32)
            piles[lot, :tall] = total
        total = sum(piles[lot, :tall] for lot in range(lots))
        odd = lax.broadcasted_iota(jnp.int32, (tall, slots), 0) % pair
        total = functools.reduce(
            lambda kept, j: jnp.where(odd == j, total[:, j * slots : (j + 1) * slots], kept),
            range(1, pair),
            total[:, :slots],
        )
        rows = [total[k * cells : (k + 1) * cells] for k in range(2 * len(kinds))]
        return [rows[2 * k] + rows[2 * k + 1] for k in range(len(kinds))]

    pair = 2 if cells % 2 == 0 else 1
    lots = 2 if cells % 4 == 0 else 1

    def land(kind):
        arrive(kind, ext, sizes, sent, landed)

    def land_gain(kind):
        arrive(kind, gain_ext, sizes, sent, gain_landed)

    dense[...] = jnp.zeros_like(dense)
    inner_columns(prepare)
    tabulate.wait()
    middle_cells(density)
    land(0)
    end_columns(prepare)
    end_cells(density)
    land(1)
    plane_columns(prepare)
    all_cells(density, 1)
    land(2)
    face_columns(prepare)
    all_cells(density, 2)
    land(3)
    edge_columns(prepare)
    last_cells(density, 3)

    rho_rows = sorted_rows(1)[0]
    first = jnp.maximum(rho_rows - 1.0, 0.0)
    fprime = -0.5 * EMBED_SCALE * lax.rsqrt(first + 1.0)
    gain = 0.5 - fprime * (0.5 / PAIR_SCALE)
    gain_rows = unsort([gain])[0]
    gain_own[...] = gain_rows.reshape(sizes + (1, slots))
    send_rims(mesh_counts, gain_own, gain_ext, sent, gain_landed)
    gain_ext[inner] = gain_rows.reshape(sizes + (1, slots))
    tall = [piece.astype(jnp.float32) for piece in halves(gain)]
    tall += [jnp.zeros((slots - 2 * cells, depth), jnp.float32)]
    tall = jnp.concatenate(tall, axis=0)
    tall = jnp.concatenate([tall, jnp.zeros((slots, -depth % 128), jnp.float32)], axis=1)
    standing = tall.T[:depth].astype(jnp.bfloat16)
    pick_row = lax.broadcasted_iota(jnp.int32, (slots, pair * slots), 0)
    pick_cell = jnp.where(
        pick_row < 2 * cells, pick_row - jnp.where(pick_row >= cells, cells, 0), -1
    )
    pick_lane = lax.broadcasted_iota(jnp.int32, (slots, pair * slots), 1) // slots
    for i in range(cells // pair):
        chosen = jnp.where(pick_cell == pair * i + pick_lane, 1.0, 0.0).astype(jnp.bfloat16)
        spread = jnp.dot(standing, chosen, preferred_element_type=jnp.float32)
        for j in range(pair):
            for g in range(group_count):
                lanes_of[held_at(pair * i + j, g, 3)] = spread[
                    g * ROWS : (g + 1) * ROWS, j * slots : (j + 1) * slots
                ]

    last_cells(quartics)
    inner_columns(prepare_gain)
    middle_cells(force)
    land_gain(0)
    end_columns(prepare_gain)
    end_cells(force)
    land_gain(1)
    plane_columns(prepare_gain)
    all_cells(force, 1)
    land_gain(2)
    face_columns(prepare_gain)
    all_cells(force, 2)
    land_gain(3)
    edge_columns(prepare_gain)
    last_cells(force, 3)

    scale = FORCE_SCALE * 4.0 * PAIR_SCALE
    *pushes, quartic_rows = sorted_rows(4)
    second = jnp.maximum(quartic_rows - 1.0, 0.0)
    pair_sum = PAIR_SCALE * (second - 2.0 * first)
    energy = -EMBED_SCALE * jnp.sqrt(first + 1.0) + 0.5 * pair_sum
    *pushes, energy_rows = unsort(pushes + [energy])
    energy_ref[...] = jnp.where(filled, energy_rows, 0.0).reshape(sizes + (slots,))
    for k, push in enumerate(pushes):
        force_ref[k] = jnp.where(filled, scale * push, 0.0).reshape(sizes + (slots,))


def groups_of(slots):
    return (slots + OCTANTS * (ROWS - 1)) // ROWS


def hand_over(energy, force, energy_out, force_out, done):
    copies = [
        pltpu.make_async_copy(force, force_out, done.at[0]),
        pltpu.make_async_copy(energy, energy_out, done.at[1]),
    ]
    for copy in copies:
        copy.start()
    for copy in copies:
        copy.wait()


def per_device(mesh_counts, positions, counts):
    slots = positions.shape[-1]
    sizes = positions.shape[1:4]
    wide = tuple(size + 2 for size in sizes)
    cells = sizes[0] * sizes[1] * sizes[2]
    far_cells = wide[0] * wide[1] * wide[2]
    groups = groups_of(slots)
    depth = -(-groups // 2) * 2 * ROWS
    f32, bf16, i32 = jnp.float32, jnp.bfloat16, jnp.int32
    roomy = 2 * cells * groups * -(-SLOTS // 3) * 16 * ROWS * slots <= 40 << 20
    quads = -(-SLOTS // (3 if roomy else 4))
    vmem = [
        ((3,) + sizes + (slots,), f32),
        ((3,) + sizes + (1, slots), f32),
        ((3,) + wide + (1, slots), f32),
        (sizes + (1, slots), f32),
        (wide + (1, slots), f32),
        ((cells, slots), i32),
        ((3, 4, cells, slots), f32),
        ((cells, depth, slots), bf16),
        ((far_cells, 4, ROWS, slots), f32),
        ((cells, groups, quads, 4, ROWS, slots), f32),
        ((cells, groups, quads, 4, ROWS, slots), f32),
        ((-(-depth // 128) * 128, slots), f32),
        ((2, 8 * cells, 2 * slots), f32),
        ((cells, slots), i32),
    ]
    held = sum(math.prod(shape) * jnp.dtype(kind).itemsize for shape, kind in vmem)
    results = pl.pallas_call(
        functools.partial(kernel, mesh_counts),
        out_shape=(
            jax.ShapeDtypeStruct(sizes + (slots,), f32),
            jax.ShapeDtypeStruct((3,) + sizes + (slots,), f32),
        ),
        in_specs=[pl.BlockSpec(memory_space=pltpu.HBM)] * 2,
        out_specs=(pl.BlockSpec(memory_space=pltpu.VMEM),) * 2,
        scratch_shapes=[pltpu.SMEM(counts.shape, i32)]
        + [pltpu.VMEM(shape, kind) for shape, kind in vmem]
        + [
            pltpu.SMEM((cells, slots), i32),
            pltpu.SemaphoreType.DMA((2,)),
            pltpu.SemaphoreType.DMA,
        ]
        + [pltpu.SemaphoreType.DMA((4,))] * 3,
        compiler_params=pltpu.CompilerParams(
            collective_id=0,
            has_side_effects=True,
            vmem_limit_bytes=held + (4 << 20),
        ),
        name="atoms",
    )(*(pltpu.with_memory_space_constraint(x, pltpu.HBM) for x in (counts, positions)))
    return pl.pallas_call(
        hand_over,
        out_shape=tuple(jax.ShapeDtypeStruct(x.shape, x.dtype) for x in results),
        in_specs=[pl.BlockSpec(memory_space=pltpu.VMEM)] * 2,
        out_specs=(pl.BlockSpec(memory_space=pl.ANY),) * 2,
        scratch_shapes=[pltpu.SemaphoreType.DMA((2,))],
        compiler_params=pltpu.CompilerParams(vmem_limit_bytes=1 << 20),
        name="hand",
    )(*results)


def solution(mesh):
    placed = (P(None, "gx", "gy", "gz", None), P("gx", "gy", "gz"))
    return jax.shard_map(
        functools.partial(per_device, tuple(mesh.shape[name] for name in NAMES)),
        mesh=mesh,
        in_specs=placed,
        out_specs=(P("gx", "gy", "gz", None), P(None, "gx", "gy", "gz", None)),
        check_vma=False,
    )
```
